16 devices in a mesh: dp: 2 (over z), ep: 8 (over y, x, core).
Axes of the slice: x: 2, y: 2, z: 2, core: 2. Of those that a mesh axis runs over, the one named last changes fastest.
Arguments:
- x_tokens: bfloat16 [131072, 768], P(('dp', 'ep'))
- modality: int32 [131072], P(('dp', 'ep'))
- router: float32 [768, 16], replicated
- expert_ids: int32 [131072], P(('dp', 'ep'))
- priority: int32 [131072], P(('dp', 'ep'))
- w_in: bfloat16 [16, 768, 3072], P('ep')
- b_in: bfloat16 [16, 3072], P('ep')
- w_out: bfloat16 [16, 3072, 768], P('ep')
- b_out: bfloat16 [16, 768], P('ep')
- dy_out: bfloat16 [131072, 768], P(('dp', 'ep'))
Outputs:
- output 1: bfloat16 [131072, 768], P(('dp', 'ep'))
- output 2: float32 [], replicated
- output 3: bfloat16 [131072, 768], P(('dp', 'ep'))
- output 4: float32 [768, 16], replicated
- output 5: bfloat16 [16, 768, 3072], P('ep')
- output 6: bfloat16 [16, 3072], P('ep')
- output 7: bfloat16 [16, 3072, 768], P('ep')
- output 8: bfloat16 [16, 768], P('ep')
All inputs are finite; a program needn't handle non-finite values.
Results may differ from the reference program's by a relative error of at most 0.00946413.
Values are sent between devices in bfloat16 or wider.
A program may use at most 1 GiB of HBM per device.

```python
import jax
import jax.numpy as jnp
from jax import lax

TOKENS = 8192
WIDTH = 768
HIDDEN = 3072
EXPERTS = 16
GROUPS = 16


def setup_inputs(seed: int = 0) -> dict:
    total_tokens = TOKENS * GROUPS
    key_set = jax.random.split(jax.random.key(seed), 16)
    local_index = jnp.arange(TOKENS)[None, :]
    text_pct = jax.random.randint(key_set[0], (GROUPS, 1), 5, 41)
    modality = (jax.random.randint(key_set[1], (GROUPS, TOKENS), 0, 100) < text_pct).astype(jnp.int32)
    modality = jnp.where(local_index == 0, 0, jnp.where(local_index == 1, 1, modality))
    hot_base = jax.random.randint(key_set[2], (GROUPS, 1), 0, EXPERTS)
    hot_pick = (hot_base + jax.random.randint(key_set[3], (GROUPS, TOKENS), 0, 4)) % EXPERTS
    spread_pick = jax.random.randint(key_set[4], (GROUPS, TOKENS), 0, EXPERTS)
    use_hot = (modality == 1) & (jax.random.randint(key_set[5], (GROUPS, TOKENS), 0, 4) < 3)
    expert_ids = jnp.where(local_index < EXPERTS, local_index, jnp.where(use_hot, hot_pick, spread_pick))
    priority = jax.vmap(lambda perm_key: jax.random.permutation(perm_key, TOKENS))(jax.random.split(key_set[6], GROUPS))
    router = jax.random.normal(key_set[7], (WIDTH, EXPERTS), jnp.float32) * WIDTH ** -0.5
    boost_dir = router.T / jnp.sum(router * router, axis=0)[:, None]
    expert_onehot = (expert_ids.reshape(total_tokens, 1) == jnp.arange(EXPERTS)[None, :]).astype(jnp.float32)
    base_noise = jax.random.normal(key_set[8], (GROUPS, TOKENS, WIDTH), jnp.float32)
    group_shift = 0.5 * jax.random.normal(key_set[9], (GROUPS, 1, WIDTH), jnp.float32)
    text_shift = 0.5 * jax.random.normal(key_set[10], (WIDTH,), jnp.float32)
    x_tokens = (base_noise + group_shift + modality[:, :, None] * text_shift).reshape(total_tokens, WIDTH)
    x_tokens = x_tokens + 4.0 * jnp.dot(expert_onehot, boost_dir)
    w_in = jax.random.normal(key_set[11], (EXPERTS, WIDTH, HIDDEN), jnp.float32) * WIDTH ** -0.5
    b_in = 0.5 * jax.random.normal(key_set[12], (EXPERTS, HIDDEN), jnp.float32)
    w_out = jax.random.normal(key_set[13], (EXPERTS, HIDDEN, WIDTH), jnp.float32) * HIDDEN ** -0.5
    b_out = 0.5 * jax.random.normal(key_set[14], (EXPERTS, WIDTH), jnp.float32)
    dy_out = jax.random.normal(key_set[15], (total_tokens, WIDTH), jnp.float32) * (total_tokens * WIDTH) ** -0.5
    return dict(
        x_tokens=x_tokens.astype(jnp.bfloat16),
        modality=modality.reshape(total_tokens).astype(jnp.int32),
        router=router,
        expert_ids=expert_ids.reshape(total_tokens).astype(jnp.int32),
        priority=priority.reshape(total_tokens).astype(jnp.int32),
        w_in=w_in.astype(jnp.bfloat16),
        b_in=b_in.astype(jnp.bfloat16),
        w_out=w_out.astype(jnp.bfloat16),
        b_out=b_out.astype(jnp.bfloat16),
        dy_out=dy_out.astype(jnp.bfloat16),
    )


def route_group(expert_ids, priority):
    capacity = TOKENS // EXPERTS
    sort_order = jnp.argsort(expert_ids * TOKENS + priority)
    sorted_rank = jnp.argsort(sort_order)
    counts = jnp.sum((expert_ids[:, None] == jnp.arange(EXPERTS)[None, :]).astype(jnp.int32), axis=0)
    starts = jnp.cumsum(counts) - counts
    slot_rank = jnp.arange(capacity)
    slot_token = sort_order[jnp.minimum(starts[:, None] + slot_rank[None, :], TOKENS - 1)]
    slot_valid = slot_rank[None, :] < counts[:, None]
    position = sorted_rank - starts[expert_ids]
    return slot_token, slot_valid, position


def expert_block(operands):
    slot_rows, w_first, b_first, w_second, b_second = operands
    act_in = jnp.dot(slot_rows, w_first, preferred_element_type=jnp.float32) + b_first.astype(jnp.float32)
    hidden = jax.nn.gelu(act_in).astype(jnp.bfloat16)
    expert_out = jnp.dot(hidden, w_second, preferred_element_type=jnp.float32) + b_second.astype(jnp.float32)
    return expert_out.astype(jnp.bfloat16)


def reference(x_tokens, modality, router, expert_ids, priority, w_in, b_in, w_out, b_out, dy_out):
    total_tokens = x_tokens.shape[0]
    groups = total_tokens // TOKENS
    capacity = TOKENS // EXPERTS
    slot_token, slot_valid, position = jax.vmap(route_group)(expert_ids.reshape(groups, TOKENS), priority.reshape(groups, TOKENS))
    group_base = jnp.arange(groups)[:, None, None] * TOKENS
    slot_global = jnp.transpose(slot_token + group_base, (1, 0, 2)).reshape(EXPERTS, groups * capacity)
    valid_global = jnp.transpose(slot_valid, (1, 0, 2)).reshape(EXPERTS, groups * capacity, 1)
    position = position.reshape(total_tokens)
    keep_mask = (position < capacity)[:, None]
    group_of = jnp.arange(total_tokens) // TOKENS
    token_slot = expert_ids * (groups * capacity) + group_of * capacity + jnp.minimum(position, capacity - 1)
    expert_onehot = (expert_ids[:, None] == jnp.arange(EXPERTS)[None, :]).astype(jnp.float32)
    mod_mask = jnp.stack([modality == 0, modality == 1]).astype(jnp.float32)
    mod_count = jnp.sum(mod_mask, axis=1)

    def forward(x_in, router_in, w_first, b_first, w_second, b_second):
        logits = jnp.dot(x_in.astype(jnp.float32), router_in)
        log_probs = jax.nn.log_softmax(logits, axis=-1)
        router_probs = jnp.exp(log_probs)
        gate_prob = jnp.sum(router_probs * expert_onehot, axis=-1, keepdims=True)
        entropy = -jnp.sum(router_probs * log_probs, axis=-1)
        mean_probs = jnp.dot(mod_mask, router_probs) / mod_count[:, None]
        aux_loss = jnp.sum(jnp.dot(mod_mask, entropy) / mod_count) + jnp.sum(mean_probs * jnp.log(mean_probs))
        gathered = jnp.where(valid_global, x_in[slot_global], 0.0).astype(x_in.dtype)
        expert_out = lax.map(jax.checkpoint(expert_block), (gathered, w_first, b_first, w_second, b_second))
        y_tok = expert_out.reshape(EXPERTS * groups * capacity, WIDTH)[token_slot]
        out_tokens = jnp.where(keep_mask, gate_prob * y_tok.astype(jnp.float32), 0.0).astype(jnp.bfloat16)
        return out_tokens, aux_loss

    (out_tokens, aux_loss), pullback = jax.vjp(forward, x_tokens, router, w_in, b_in, w_out, b_out)
    dx_tokens, d_router, d_w_in, d_b_in, d_w_out, d_b_out = pullback((dy_out, jnp.ones_like(aux_loss)))
    return out_tokens, aux_loss, dx_tokens, d_router, d_w_in, d_b_in, d_w_out, d_b_out
```

```python
import functools
import jax
import jax.numpy as jnp
from jax import lax
from jax.experimental import pallas as pl
from jax.experimental.pallas import tpu as pltpu
from jax.sharding import PartitionSpec as P

F32 = jnp.float32
BF16 = jnp.bfloat16
VMEM_CAP = 66_000_000
GELU_SCALE = 0.7978845608028654
GELU_CUBE = 0.044715
FCHUNK = 768


def gelu_and_slope(a):
    sq = a * a
    t = jnp.tanh(GELU_SCALE * (a + GELU_CUBE * (a * sq)))
    cdf = 0.5 * (1.0 + t)
    slope = cdf + (0.5 * a) * ((1.0 - t * t) * (GELU_SCALE * (1.0 + (3.0 * GELU_CUBE) * sq)))
    return a * cdf, slope


def expert_body(want_rows, dw_in_init, dw_final, nsteps, fchunk, *refs):
    it = iter(refs)
    sel_ref = next(it)
    x_ref, d_ref, w1_ref, b1_ref, w2_ref, b2_ref = (next(it) for _ in range(6))
    want_dw = dw_final is not None
    if dw_in_init:
        p1_ref, p2_ref, pb1_ref, pb2_ref = (next(it) for _ in range(4))
    if want_rows:
        y_ref, dx_ref = next(it), next(it)
    if want_dw:
        g1_ref, g2_ref, gb1_ref, gb2_ref = (next(it) for _ in range(4))
        acc1, acc2, xt, dt, sem = (next(it) for _ in range(5))
        if dw_final:
            stage = next(it)
    if want_rows:
        yacc, dxacc = next(it), next(it)
    step = pl.program_id(0)
    width = x_ref.shape[-1]
    hidden = w1_ref.shape[-1]
    x = x_ref[...].reshape(-1, width)
    d = d_ref[...].reshape(-1, width)
    if want_dw:
        @pl.when(step == 0)
        def _():
            if dw_in_init:
                c1 = pltpu.make_async_copy(p1_ref, acc1, sem.at[0])
                c2 = pltpu.make_async_copy(p2_ref, acc2, sem.at[1])
                c1.start()
                c2.start()
                gb1_ref[...] = pb1_ref[...]
                gb2_ref[...] = pb2_ref[...]
                c1.wait()
                c2.wait()
            else:
                acc1[...] = jnp.zeros_like(acc1)
                acc2[...] = jnp.zeros_like(acc2)
                gb1_ref[...] = jnp.zeros_like(gb1_ref)
                gb2_ref[...] = jnp.zeros_like(gb2_ref)

        xt[...] = x.T
        dt[...] = d.T
        gb2_ref[...] += jnp.sum(d.astype(F32), axis=0, keepdims=True)
    if want_rows:
        yacc[...] = jnp.broadcast_to(b2_ref[0].astype(F32), yacc.shape)
        dxacc[...] = jnp.zeros_like(dxacc)

    def chunk(j, carry):
        cols = pl.ds(pl.multiple_of(j * fchunk, fchunk), fchunk)
        w1 = w1_ref[0, :, cols]
        w2 = w2_ref[0, cols, :]
        a = jnp.dot(x, w1, preferred_element_type=F32) + b1_ref[0, :, cols].astype(F32)
        dh = lax.dot_general(d, w2, (((1,), (1,)), ((), ())), preferred_element_type=F32)
        h, slope = gelu_and_slope(a)
        da = dh.astype(BF16).astype(F32) * slope
        h16 = h.astype(BF16)
        da16 = da.astype(BF16)
        if want_rows:
            yacc[...] += jnp.dot(h16, w2, preferred_element_type=F32)
            dxacc[...] += lax.dot_general(da16, w1, (((1,), (1,)), ((), ())), preferred_element_type=F32)
        if want_dw:
            gb1_ref[:, cols] += jnp.sum(da, axis=0, keepdims=True)
            acc1[:, cols] += jnp.dot(xt[...], da16, preferred_element_type=F32)
            acc2[:, cols] += jnp.dot(dt[...], h16, preferred_element_type=F32)
        return carry

    lax.fori_loop(0, hidden // fchunk, chunk, 0)
    if want_rows:
        y_ref[...] = yacc[...].astype(BF16).reshape(y_ref.shape)
        dx_ref[...] = dxacc[...].astype(BF16).reshape(dx_ref.shape)
    if want_dw:
        @pl.when(step == nsteps - 1)
        def _():
            if dw_final:
                def put(j, carry):
                    cols = pl.ds(pl.multiple_of(j * fchunk, fchunk), fchunk)
                    stage[...] = acc2[:, cols].T.astype(BF16)
                    c = pltpu.make_async_copy(stage, g2_ref.at[cols, :], sem.at[1])
                    c.start()
                    c.wait()
                    stage[...] = acc1[:, cols].astype(BF16)
                    c = pltpu.make_async_copy(stage, g1_ref.at[:, cols], sem.at[0])
                    c.start()
                    c.wait()
                    return carry

                lax.fori_loop(0, hidden // fchunk, put, 0)
            else:
                c1 = pltpu.make_async_copy(acc1, g1_ref, sem.at[0])
                c2 = pltpu.make_async_copy(acc2, g2_ref, sem.at[1])
                c1.start()
                c2.start()
                c1.wait()
                c2.wait()


def expert_call(sel, rows, cots, w1, b1, w2, b2, partial=None, want_rows=True, dw=None, fchunk=FCHUNK):
    tiles, r, width = rows.shape
    hidden = w1.shape[-1]
    one = pl.Buffered(1)
    tile = pl.BlockSpec((1, r, width), lambda i, s: (i, 0, 0))
    anyspec = pl.BlockSpec(memory_space=pl.ANY)
    vec1 = pl.BlockSpec((1, hidden), lambda i, s: (0, 0))
    vec2 = pl.BlockSpec((1, width), lambda i, s: (0, 0))
    in_specs = [
        tile, tile,
        pl.BlockSpec((1, width, hidden), lambda i, s: (s[0], 0, 0), pipeline_mode=one),
        pl.BlockSpec((1, 1, hidden), lambda i, s: (s[0], 0, 0)),
        pl.BlockSpec((1, hidden, width), lambda i, s: (s[0], 0, 0), pipeline_mode=one),
        pl.BlockSpec((1, 1, width), lambda i, s: (s[0], 0, 0)),
    ]
    args = [rows, cots, w1, b1[:, None, :], w2, b2[:, None, :]]
    if partial is not None:
        in_specs += [anyspec, anyspec, vec1, vec2]
        args += list(partial)
    out_shape, out_specs, scratch = [], [], []
    if want_rows:
        out_shape += [jax.ShapeDtypeStruct(rows.shape, BF16)] * 2
        out_specs += [tile, tile]
    if dw:
        t = F32 if dw == "partial" else BF16
        g2 = (width, hidden) if dw == "partial" else (hidden, width)
        out_shape += [jax.ShapeDtypeStruct((width, hidden), t), jax.ShapeDtypeStruct(g2, t),
                      jax.ShapeDtypeStruct((1, hidden), F32), jax.ShapeDtypeStruct((1, width), F32)]
        out_specs += [anyspec, anyspec, vec1, vec2]
        scratch += [pltpu.VMEM((width, hidden), F32), pltpu.VMEM((width, hidden), F32),
                    pltpu.VMEM((width, r), BF16), pltpu.VMEM((width, r), BF16), pltpu.SemaphoreType.DMA((2,))]
        if dw == "final":
            assert fchunk == width
            scratch += [pltpu.VMEM((fchunk, width), BF16)]
    if want_rows:
        scratch += [pltpu.VMEM((r, width), F32), pltpu.VMEM((r, width), F32)]
    dots = 2 + 2 * bool(want_rows) + 2 * bool(dw)
    flops = dots * 2 * tiles * r * width * hidden
    body = functools.partial(expert_body, want_rows, partial is not None, None if not dw else dw == "final", tiles, fchunk)
    return pl.pallas_call(
        body,
        grid_spec=pltpu.PrefetchScalarGridSpec(num_scalar_prefetch=1, grid=(tiles,), in_specs=in_specs, out_specs=out_specs, scratch_shapes=scratch),
        out_shape=out_shape,
        compiler_params=pltpu.CompilerParams(vmem_limit_bytes=VMEM_CAP, dimension_semantics=("arbitrary",)),
        cost_estimate=pl.CostEstimate(flops=flops, bytes_accessed=4 * tiles * r * width * 2, transcendentals=tiles * r * hidden),
        name="expert_" + ("rows" if want_rows else "") + (dw or ""),
    )(sel, *args)


ALL_AXES = ("dp", "ep")
MESH_ID = pl.DeviceIdType.MESH


def slots_kernel(num_tokens, capacity, scal_ref, order_ref, xs_ref, ds_ref):
    mine = lax.axis_index("dp")
    experts = xs_ref.shape[0] * 128 // capacity
    rows = capacity // 128
    lane = lax.broadcasted_iota(jnp.int32, (rows, 128), 1)
    rank = lax.broadcasted_iota(jnp.int32, (rows, 128), 0) * 128 + lane
    for j in range(experts):
        owner = (1 - mine) if j < experts // 2 else mine
        e = 2 * (j % (experts // 2)) + owner
        start = scal_ref[e]
        count = scal_ref[experts + e]
        block = order_ref[pl.ds(start // 128, 8), :]
        off = lax.rem(start, 128)
        turned = pltpu.roll(block, lax.rem(128 - off, 128), 1)
        tok = jnp.where(lane < 128 - off, turned[:rows], turned[1:rows + 1])
        xs_ref[rows * j:rows * (j + 1), :] = jnp.where(rank < count, tok, 0)
        ds_ref[rows * j:rows * (j + 1), :] = jnp.where(rank < count, tok, num_tokens)


def slot_tables(order, starts, counts, capacity):
    num_tokens = order.shape[0]
    experts = starts.shape[0]
    padded = jnp.pad(order, (0, 1024)).reshape(-1, 128)
    shape = jax.ShapeDtypeStruct((experts * capacity // 128, 128), jnp.int32)
    xs, ds = pl.pallas_call(
        functools.partial(slots_kernel, num_tokens, capacity),
        in_specs=[pl.BlockSpec(memory_space=pltpu.SMEM), pl.BlockSpec(memory_space=pltpu.VMEM)],
        out_specs=[pl.BlockSpec(memory_space=pltpu.VMEM)] * 2,
        out_shape=[shape, shape],
        cost_estimate=pl.CostEstimate(flops=1_000_000, bytes_accessed=200_000, transcendentals=0),
        name="slots",
    )(jnp.concatenate([starts, counts]), padded)
    half = experts * capacity // 2
    xs, ds = xs.reshape(-1), ds.reshape(-1)
    return (xs[:half], xs[half:]), (ds[:half], ds[half:])


def sum_kernel(ep_size, count, x_ref, out_ref, slots, send_sem, recv_sem):
    dp_me, ep_me = lax.axis_index("dp"), lax.axis_index("ep")
    me = dp_me * ep_size + ep_me

    def peer(k):
        p = lax.rem(me + k, count)
        return (p // ep_size, lax.rem(p, ep_size))

    barrier = pltpu.get_barrier_semaphore()
    for k in range(1, count):
        pl.semaphore_signal(barrier, inc=1, device_id=peer(k), device_id_type=MESH_ID)
    pl.semaphore_wait(barrier, count - 1)
    copies = []
    for k in range(1, count):
        c = pltpu.make_async_remote_copy(
            src_ref=x_ref, dst_ref=slots.at[me], send_sem=send_sem.at[k], recv_sem=recv_sem.at[k],
            device_id=peer(k), device_id_type=MESH_ID)
        c.start()
        copies.append(c)
    slots[me] = x_ref[...]
    for c in copies:
        c.wait()
    total = slots[0]
    for k in range(1, count):
        total = total + slots[k]
    out_ref[...] = total


def device_sum(x, mesh, collective_id):
    count = mesh.shape["dp"] * mesh.shape["ep"]
    return pl.pallas_call(
        functools.partial(sum_kernel, mesh.shape["ep"], count),
        in_specs=[pl.BlockSpec(memory_space=pltpu.VMEM)],
        out_specs=pl.BlockSpec(memory_space=pltpu.VMEM),
        out_shape=jax.ShapeDtypeStruct(x.shape, F32),
        scratch_shapes=[pltpu.VMEM((count,) + x.shape, F32), pltpu.SemaphoreType.DMA((count,)), pltpu.SemaphoreType.DMA((count,))],
        compiler_params=pltpu.CompilerParams(collective_id=collective_id, has_side_effects=True),
        cost_estimate=pl.CostEstimate(flops=10_000_000, bytes_accessed=1_000_000, transcendentals=0),
        name="device_sum",
    )(x)


def exchange_body(ep_size, count, fchunk,
                  xs, ds, xo, do, w1_hbm, w2_hbm, b1_ref, b2_ref, st_ref,
                  yb, dxb, g1_ref, g2_ref, gb1_ref, gb2_ref, st_out, xr, dr, xf, df, yl, dxl,
                  w1, w2, acc1, acc2, xv, dv, xt, dt, yacc, dxacc, ystage, dxstage, stage, slots,
                  st_send, st_recv, x_send, x_recv, d_send, d_recv, xf_send, xf_recv, df_send, df_recv,
                  y_send, y_recv, dx_send, dx_recv, w_sem, in_sem, out_sem):
    width = w1.shape[0]
    hidden = w1.shape[1]
    mine, e = lax.axis_index("dp"), lax.axis_index("ep")
    me = mine * ep_size + e

    def anyone(k):
        p = lax.rem(me + k, count)
        return (p // ep_size, lax.rem(p, ep_size))

    def dest(k):
        return lax.rem(e + k, ep_size)

    def source(k):
        return lax.rem(e + ep_size - k, ep_size)

    def remote(src, dst, send, recv, dp, ep):
        return pltpu.make_async_remote_copy(src_ref=src, dst_ref=dst, send_sem=send, recv_sem=recv,
                                            device_id=(dp, ep), device_id_type=MESH_ID)

    def stat_copy(k):
        dp, ep = anyone(k)
        return remote(st_ref, slots.at[me], st_send.at[k], st_recv.at[k], dp, ep)

    def x_copy(k):
        return remote(xs.at[dest(k)], xr.at[e], x_send.at[k], x_recv.at[k], mine, dest(k))

    def d_copy(k):
        return remote(ds.at[dest(k)], dr.at[e], d_send.at[k], d_recv.at[k], mine, dest(k))

    def xf_copy(t):
        return remote(xo.at[t], xf.at[t], xf_send.at[t], xf_recv.at[t], 1 - mine, e)

    def df_copy(t):
        return remote(do.at[t], df.at[t], df_send.at[t], df_recv.at[t], 1 - mine, e)

    def y_copy(k):
        return remote(yl.at[source(k)], yb.at[e], y_send.at[k], y_recv.at[k], mine, source(k))

    def dx_copy(k):
        return remote(dxl.at[source(k)], dxb.at[e], dx_send.at[k], dx_recv.at[k], mine, source(k))

    load1 = pltpu.make_async_copy(w1_hbm.at[mine], w1, w_sem.at[0])
    load2 = pltpu.make_async_copy(w2_hbm.at[mine], w2, w_sem.at[1])
    load1.start()
    load2.start()
    barrier = pltpu.get_barrier_semaphore()
    for k in range(1, count):
        pl.semaphore_signal(barrier, inc=1, device_id=anyone(k), device_id_type=MESH_ID)
    pl.semaphore_wait(barrier, count - 1)
    for k in range(1, count):
        stat_copy(k).start()
    for k in range(1, ep_size):
        x_copy(k).start()
        d_copy(k).start()
    for t in range(ep_size):
        xf_copy(t).start()
        df_copy(t).start()
    slots[me] = st_ref[...]
    acc1[...] = jnp.zeros_like(acc1)
    acc2[...] = jnp.zeros_like(acc2)
    gb1_ref[...] = jnp.zeros_like(gb1_ref)
    gb2_ref[...] = jnp.zeros_like(gb2_ref)

    def fetch(x_src, d_src, slot):
        return (pltpu.make_async_copy(x_src, xv.at[slot], in_sem.at[0, slot]),
                pltpu.make_async_copy(d_src, dv.at[slot], in_sem.at[1, slot]))

    def start_all(copies):
        for c in copies:
            c.start()

    def wait_all(copies):
        for c in copies:
            c.wait()

    def tile(slot, want_rows):
        x, d = xv[slot], dv[slot]
        xt[...] = x.T
        dt[...] = d.T
        gb2_ref[...] += jnp.sum(d.astype(F32), axis=0, keepdims=True)
        if want_rows:
            yacc[...] = jnp.broadcast_to(b2_ref[mine].astype(F32), yacc.shape)
            dxacc[...] = jnp.zeros_like(dxacc)

        def chunk(j, carry):
            cols = pl.ds(pl.multiple_of(j * fchunk, fchunk), fchunk)
            w1c = w1[:, cols]
            w2c = w2[cols, :]
            a = jnp.dot(x, w1c, preferred_element_type=F32) + b1_ref[mine, :, cols].astype(F32)
            dh = lax.dot_general(d, w2c, (((1,), (1,)), ((), ())), preferred_element_type=F32)
            h, slope = gelu_and_slope(a)
            da = dh.astype(BF16).astype(F32) * slope
            h16 = h.astype(BF16)
            da16 = da.astype(BF16)
            if want_rows:
                yacc[...] += jnp.dot(h16, w2c, preferred_element_type=F32)
                dxacc[...] += lax.dot_general(da16, w1c, (((1,), (1,)), ((), ())), preferred_element_type=F32)
            gb1_ref[:, cols] += jnp.sum(da, axis=0, keepdims=True)
            acc1[:, cols] += jnp.dot(xt[...], da16, preferred_element_type=F32)
            acc2[:, cols] += jnp.dot(dt[...], h16, preferred_element_type=F32)
            return carry

        lax.fori_loop(0, hidden // fchunk, chunk, 0)

    first = fetch(xs.at[e], ds.at[e], 0)
    start_all(first)
    load1.wait()
    load2.wait()
    wait_all(first)

    def near_step(k, carry):
        slot = lax.rem(k, 2)
        src = source(k)

        @pl.when(k > 0)
        def _():
            wait_all(fetch(xr.at[src], dr.at[src], slot))

        tile(slot, True)

        @pl.when(k < ep_size - 1)
        def _():
            x_copy(k + 1).wait_recv()
            d_copy(k + 1).wait_recv()
            start_all(fetch(xr.at[source(k + 1)], dr.at[source(k + 1)], lax.rem(k + 1, 2)))

        @pl.when(k == ep_size - 1)
        def _():
            xf_copy(0).wait_recv()
            df_copy(0).wait_recv()
            start_all(fetch(xf.at[0], df.at[0], 0))

        ystage[...] = yacc[...].astype(BF16)
        dxstage[...] = dxacc[...].astype(BF16)

        @pl.when(k == 0)
        def _():
            out = (pltpu.make_async_copy(ystage, yb.at[e], out_sem.at[0]), pltpu.make_async_copy(dxstage, dxb.at[e], out_sem.at[1]))
            start_all(out)
            wait_all(out)

        @pl.when(k > 0)
        def _():
            out = (pltpu.make_async_copy(ystage, yl.at[src], out_sem.at[0]), pltpu.make_async_copy(dxstage, dxl.at[src], out_sem.at[1]))
            start_all(out)
            wait_all(out)
            y_copy(k).start()
            dx_copy(k).start()

        return carry

    lax.fori_loop(0, ep_size, near_step, 0)

    def far_step(t, carry):
        slot = lax.rem(t, 2)
        wait_all(fetch(xf.at[t], df.at[t], slot))

        tile(slot, False)

        @pl.when(t < ep_size - 1)
        def _():
            xf_copy(t + 1).wait_recv()
            df_copy(t + 1).wait_recv()
            start_all(fetch(xf.at[t + 1], df.at[t + 1], lax.rem(t + 1, 2)))

        return carry

    lax.fori_loop(0, ep_size, far_step, 0)

    def put(j, carry):
        cols = pl.ds(pl.multiple_of(j * fchunk, fchunk), fchunk)
        stage[0] = acc2[:, cols].T.astype(BF16)
        c2 = pltpu.make_async_copy(stage.at[0], g2_ref.at[cols, :], out_sem.at[1])
        c2.start()
        stage[1] = acc1[:, cols].astype(BF16)
        c1 = pltpu.make_async_copy(stage.at[1], g1_ref.at[:, cols], out_sem.at[0])
        c1.start()
        c2.wait()
        c1.wait()
        return carry

    lax.fori_loop(0, hidden // fchunk, put, 0)
    for k in range(1, count):
        stat_copy(k).wait()
    total = slots[0]
    for k in range(1, count):
        total = total + slots[k]
    st_out[...] = total
    for t in range(ep_size):
        xf_copy(t).wait_send()
        df_copy(t).wait_send()
    for k in range(1, ep_size):
        x_copy(k).wait_send()
        d_copy(k).wait_send()
        y_copy(k).wait()
        dx_copy(k).wait()


def exchange_call(mesh, xs, ds, xo, do, w1, b1, w2, b2, stats, fchunk=FCHUNK):
    ep_size = mesh.shape["ep"]
    count = mesh.shape["dp"] * ep_size
    tiles, r, width = xs.shape
    hidden = w1.shape[-1]
    anyspec = pl.BlockSpec(memory_space=pl.ANY)
    vm = pl.BlockSpec(memory_space=pltpu.VMEM)
    rows = jax.ShapeDtypeStruct(xs.shape, BF16)
    out_shape = [rows, rows, jax.ShapeDtypeStruct((width, hidden), BF16), jax.ShapeDtypeStruct((hidden, width), BF16),
                 jax.ShapeDtypeStruct((1, hidden), F32), jax.ShapeDtypeStruct((1, width), F32), jax.ShapeDtypeStruct(stats.shape, F32)] + [rows] * 6
    out_specs = [anyspec] * 4 + [vm] * 3 + [anyspec] * 6
    dma = pltpu.SemaphoreType.DMA
    scratch = [
        pltpu.VMEM((width, hidden), BF16), pltpu.VMEM((hidden, width), BF16),
        pltpu.VMEM((width, hidden), F32), pltpu.VMEM((width, hidden), F32),
        pltpu.VMEM((2, r, width), BF16), pltpu.VMEM((2, r, width), BF16),
        pltpu.VMEM((width, r), BF16), pltpu.VMEM((width, r), BF16),
        pltpu.VMEM((r, width), F32), pltpu.VMEM((r, width), F32),
        pltpu.VMEM((r, width), BF16), pltpu.VMEM((r, width), BF16),
        pltpu.VMEM((2, fchunk, width), BF16), pltpu.VMEM((count,) + stats.shape, F32),
        dma((count,)), dma((count,)),
    ] + [dma((ep_size,))] * 12 + [dma((2,)), dma((2, 2)), dma((2,))]
    flops = 10 * 2 * tiles * r * width * hidden
    return pl.pallas_call(
        functools.partial(exchange_body, ep_size, count, fchunk),
        in_specs=[anyspec] * 6 + [vm] * 3,
        out_specs=out_specs,
        out_shape=out_shape,
        scratch_shapes=scratch,
        compiler_params=pltpu.CompilerParams(vmem_limit_bytes=VMEM_CAP, collective_id=1, has_side_effects=True),
        cost_estimate=pl.CostEstimate(flops=flops, bytes_accessed=8 * tiles * r * width * 2, transcendentals=2 * tiles * r * hidden),
        name="exchange",
    )(xs, ds, xo, do, w1, w2, b1[:, None, :], b2[:, None, :], stats)[:7]


def router_forward(x_loc, modality, router, expert_ids):
    num_experts = router.shape[1]
    logits = jnp.dot(x_loc, router, precision=lax.Precision.HIGHEST, preferred_element_type=F32)
    log_probs = jax.nn.log_softmax(logits, axis=-1)
    router_probs = jnp.exp(log_probs)
    expert_onehot = (expert_ids[:, None] == jnp.arange(num_experts)[None, :]).astype(F32)
    gate_prob = jnp.sum(router_probs * expert_onehot, axis=-1)
    mod_mask = jnp.stack([modality == 0, modality == 1]).astype(F32)
    entropy = -jnp.sum(router_probs * log_probs, axis=-1)
    local_stats = jnp.concatenate([jnp.dot(mod_mask, router_probs), jnp.dot(mod_mask, entropy)[:, None], jnp.sum(mod_mask, axis=1, keepdims=True)], axis=1)
    return log_probs, router_probs, expert_onehot, gate_prob, mod_mask, local_stats


def aux_from_stats(stats, num_experts):
    mod_count = stats[:, num_experts + 1]
    mean_probs = stats[:, :num_experts] / mod_count[:, None]
    aux_loss = jnp.sum(stats[:, num_experts] / mod_count) + jnp.sum(mean_probs * jnp.log(mean_probs))
    return aux_loss, mean_probs, mod_count


def router_backward(x_loc, router, log_probs, router_probs, expert_onehot, mod_mask, mean_probs, mod_count, d_gate):
    inv_count = jnp.dot(1.0 / mod_count, mod_mask)
    global_part = jnp.einsum("mt,me->te", mod_mask, jnp.log(mean_probs) / mod_count[:, None])
    d_probs = expert_onehot * d_gate[:, None] + global_part - log_probs * inv_count[:, None]
    d_logits = router_probs * (d_probs - jnp.sum(d_probs * router_probs, axis=-1, keepdims=True))
    d_router_part = jnp.einsum("tw,te->we", x_loc, d_logits, precision=lax.Precision.HIGHEST, preferred_element_type=F32)
    dx_router = jnp.einsum("te,we->tw", d_logits, router, precision=lax.Precision.HIGHEST, preferred_element_type=F32)
    return d_router_part, dx_router.astype(BF16)


def solution(mesh):
    token_spec = P(ALL_AXES)
    expert_spec = P("ep")
    swap = [(i, 1 - i) for i in range(2)]

    def local_step(x_loc, modality, router, expert_ids, priority, w_in, b_in, w_out, b_out, dy_loc):
        num_tokens, width = x_loc.shape
        num_experts = router.shape[1]
        capacity = num_tokens // num_experts
        half = num_experts // 2
        mine = lax.axis_index("dp")
        order = jnp.argsort(expert_ids * num_tokens + priority)
        counts = jnp.sum((expert_ids[:, None] == jnp.arange(num_experts)[None, :]).astype(jnp.int32), axis=0)
        starts = jnp.cumsum(counts) - counts
        x_slots, d_slots = slot_tables(order, starts, counts, capacity)

        def to_owner(table, slots):
            rows = jnp.take(table, slots, axis=0, mode="clip").reshape(half, capacity, width)
            return lax.all_to_all(rows, "ep", 0, 0, tiled=True)

        def pick(table, slots):
            return jnp.take(table, slots, axis=0, mode="clip").reshape(half, capacity, width)

        def swap_rows(rows):
            return lax.all_to_all(rows, "ep", 0, 0, tiled=True)

        x_other = swap_rows(pick(x_loc, x_slots[0]))
        log_probs, router_probs, expert_onehot, gate_prob, mod_mask, local_stats = router_forward(x_loc, modality, router, expert_ids)
        dy_f32 = dy_loc.astype(F32)
        d_tok = jnp.pad((gate_prob[:, None] * dy_f32).astype(BF16), ((0, 8), (0, 0)))
        d_other = swap_rows(pick(d_tok, d_slots[0]))
        x_send = pick(x_loc, x_slots[1])
        d_send = pick(d_tok, d_slots[1])
        stats_block = jnp.pad(local_stats, ((0, 6), (0, 128 - num_experts - 2)))
        y_mine, dx_mine, g_in, g_out, gb_in, gb_out, stats_sum = exchange_call(mesh, x_send, d_send, x_other, d_other, w_in, b_in, w_out, b_out, stats_block)
        aux_loss, mean_probs, mod_count = aux_from_stats(stats_sum[:2, :num_experts + 2], num_experts)
        sel_other = jnp.reshape(1 - mine, (1,)).astype(jnp.int32)
        sel_other, _ = lax.optimization_barrier((sel_other, stats_sum))
        g_bias = jnp.concatenate([gb_in, gb_out], axis=1).astype(BF16)
        far_out = lax.ppermute(g_out, "dp", swap)
        far_in = lax.ppermute(g_in, "dp", swap)
        far_bias = lax.ppermute(g_bias, "dp", swap)
        y_other, dx_other = expert_call(sel_other, x_other, d_other, w_in, b_in, w_out, b_out)
        y_back = [r.reshape(half * capacity, width) for r in (swap_rows(y_other), y_mine)]
        dx_back = [r.reshape(half * capacity, width) for r in (swap_rows(dx_other), dx_mine)]

        def both(near, far):
            first = mine == 0
            return jnp.stack([jnp.where(first, near, far), jnp.where(first, far, near)])

        rank = jnp.argsort(order)
        ids = jnp.arange(num_experts)
        position = rank - jnp.sum(jnp.where(expert_ids[:, None] == ids[None, :], starts[None, :], 0), axis=1)
        keep_mask = position < capacity
        place = jnp.where(lax.rem(expert_ids, 2) == mine, half, 0) + expert_ids // 2
        token_slot = place * capacity + jnp.minimum(position, capacity - 1)
        keep_col = keep_mask[:, None]

        y_tok = jnp.take(jnp.concatenate(y_back), token_slot, axis=0, mode="clip").astype(F32)
        out_tokens = jnp.where(keep_col, gate_prob[:, None] * y_tok, 0.0).astype(BF16)
        d_gate = jnp.where(keep_mask, jnp.sum(dy_f32 * y_tok, axis=-1), 0.0)
        d_router_part, dx_router = router_backward(x_loc, router, log_probs, router_probs, expert_onehot, mod_mask, mean_probs, mod_count, d_gate)
        dx_router = lax.optimization_barrier(dx_router)
        dx_expert = jnp.where(keep_col, jnp.take(jnp.concatenate(dx_back), token_slot, axis=0, mode="clip"), 0).astype(BF16)
        dx_tokens, d_router_part = lax.optimization_barrier((dx_expert + dx_router, d_router_part))
        d_router = device_sum(d_router_part.T.reshape(-1, 128), mesh, 2).reshape(num_experts, width).T
        bias = both(g_bias[0], far_bias[0])
        hidden = w_in.shape[-1]
        return (out_tokens, aux_loss, dx_tokens, d_router, both(g_in, far_in), bias[:, :hidden], both(g_out, far_out), bias[:, hidden:])

    return jax.shard_map(
        local_step,
        mesh=mesh,
        in_specs=(token_spec, token_spec, P(), token_spec, token_spec, expert_spec, expert_spec, expert_spec, expert_spec, token_spec),
        out_specs=(token_spec, P(), token_spec, P(), expert_spec, expert_spec, expert_spec, expert_spec),
        check_vma=False,
    )
```

```python
import functools
import jax
import jax.numpy as jnp
from jax import lax
from jax.experimental import pallas as pl
from jax.experimental.pallas import tpu as pltpu
from jax.sharding import PartitionSpec as P

F32 = jnp.float32
BF16 = jnp.bfloat16
VMEM_CAP = 66_000_000
GELU_SCALE = 0.7978845608028654
GELU_CUBE = 0.044715
FCHUNK = 768


def gelu_and_slope(a):
    sq = a * a
    t = jnp.tanh(GELU_SCALE * (a + GELU_CUBE * (a * sq)))
    cdf = 0.5 * (1.0 + t)
    slope = cdf + (0.5 * a) * ((1.0 - t * t) * (GELU_SCALE * (1.0 + (3.0 * GELU_CUBE) * sq)))
    return a * cdf, slope


ALL_AXES = ("dp", "ep")
MESH_ID = pl.DeviceIdType.MESH


def slots_kernel(num_tokens, capacity, scal_ref, order_ref, xs_ref, ds_ref):
    mine = lax.axis_index("dp")
    experts = xs_ref.shape[0] * 128 // capacity
    rows = capacity // 128
    lane = lax.broadcasted_iota(jnp.int32, (rows, 128), 1)
    rank = lax.broadcasted_iota(jnp.int32, (rows, 128), 0) * 128 + lane
    for j in range(experts):
        owner = (1 - mine) if j < experts // 2 else mine
        e = 2 * (j % (experts // 2)) + owner
        start = scal_ref[e]
        count = scal_ref[experts + e]
        block = order_ref[pl.ds(start // 128, 8), :]
        off = lax.rem(start, 128)
        turned = pltpu.roll(block, lax.rem(128 - off, 128), 1)
        tok = jnp.where(lane < 128 - off, turned[:rows], turned[1:rows + 1])
        xs_ref[rows * j:rows * (j + 1), :] = jnp.where(rank < count, tok, 0)
        ds_ref[rows * j:rows * (j + 1), :] = jnp.where(rank < count, tok, num_tokens)


def slot_tables(order, starts, counts, capacity):
    num_tokens = order.shape[0]
    experts = starts.shape[0]
    padded = jnp.pad(order, (0, 1024)).reshape(-1, 128)
    shape = jax.ShapeDtypeStruct((experts * capacity // 128, 128), jnp.int32)
    xs, ds = pl.pallas_call(
        functools.partial(slots_kernel, num_tokens, capacity),
        in_specs=[pl.BlockSpec(memory_space=pltpu.SMEM), pl.BlockSpec(memory_space=pltpu.VMEM)],
        out_specs=[pl.BlockSpec(memory_space=pltpu.VMEM)] * 2,
        out_shape=[shape, shape],
        cost_estimate=pl.CostEstimate(flops=1_000_000, bytes_accessed=200_000, transcendentals=0),
        name="slots",
    )(jnp.concatenate([starts, counts]), padded)
    return xs.reshape(-1), ds.reshape(-1)


def sum_kernel(ep_size, count, x_ref, out_ref, slots, send_sem, recv_sem):
    dp_me, ep_me = lax.axis_index("dp"), lax.axis_index("ep")
    me = dp_me * ep_size + ep_me

    def peer(k):
        p = lax.rem(me + k, count)
        return (p // ep_size, lax.rem(p, ep_size))

    barrier = pltpu.get_barrier_semaphore()
    for k in range(1, count):
        pl.semaphore_signal(barrier, inc=1, device_id=peer(k), device_id_type=MESH_ID)
    pl.semaphore_wait(barrier, count - 1)
    copies = []
    for k in range(1, count):
        c = pltpu.make_async_remote_copy(
            src_ref=x_ref, dst_ref=slots.at[me], send_sem=send_sem.at[k], recv_sem=recv_sem.at[k],
            device_id=peer(k), device_id_type=MESH_ID)
        c.start()
        copies.append(c)
    slots[me] = x_ref[...]
    for c in copies:
        c.wait()
    total = slots[0]
    for k in range(1, count):
        total = total + slots[k]
    out_ref[...] = total


def device_sum(x, mesh, collective_id):
    count = mesh.shape["dp"] * mesh.shape["ep"]
    return pl.pallas_call(
        functools.partial(sum_kernel, mesh.shape["ep"], count),
        in_specs=[pl.BlockSpec(memory_space=pltpu.VMEM)],
        out_specs=pl.BlockSpec(memory_space=pltpu.VMEM),
        out_shape=jax.ShapeDtypeStruct(x.shape, F32),
        scratch_shapes=[pltpu.VMEM((count,) + x.shape, F32), pltpu.SemaphoreType.DMA((count,)), pltpu.SemaphoreType.DMA((count,))],
        compiler_params=pltpu.CompilerParams(collective_id=collective_id, has_side_effects=True),
        cost_estimate=pl.CostEstimate(flops=10_000_000, bytes_accessed=1_000_000, transcendentals=0),
        name="device_sum",
    )(x)


def take_body(n_tables, n_outs, rows_in, rows_out, chunk, q_ref, *refs):
    tables, results = refs[:n_tables], refs[n_tables:n_tables + n_outs]
    wide, inbuf, outs, outbuf, in_sem, out_sem = refs[n_tables + n_outs:]
    width = inbuf.shape[-1]
    parts = width // 128
    per_table = rows_in // chunk // n_tables

    def load(c):
        t, i = c // per_table, c % per_table
        return pltpu.make_async_copy(tables[t].at[pl.ds(i * chunk, chunk), :], inbuf.at[c % 2], in_sem.at[c % 2])

    load(0).start()
    for c in range(rows_in // chunk):
        if c + 1 < rows_in // chunk:
            load(c + 1).start()
        load(c).wait()

        def widen(g, carry, c=c):
            for u in range(2):
                v = inbuf[c % 2, pl.ds(pl.multiple_of(g * 32 + u * 16, 16), 16), :].astype(F32)
                base = (c * chunk // 8 + g * 4 + u * 2) * 8 * parts
                for hh in range(2):
                    for k in range(parts):
                        wide[pl.ds(pl.multiple_of(base + (hh * parts + k) * 8, 8), 8), :] = v[hh * 8:hh * 8 + 8, k * 128:(k + 1) * 128]
            return carry

        lax.fori_loop(0, chunk // 32, widen, 0)
    wide[rows_in * parts:, :] = jnp.zeros((8 * parts, 128), F32)

    steps = rows_out // chunk // n_outs

    def fill(o, out):
        def store(c, slot):
            return pltpu.make_async_copy(outbuf.at[slot], out.at[pl.ds(c * chunk, chunk), :], out_sem.at[slot])

        def chunk_step(c, carry):
            slot = lax.rem(c, 2)

            def rows(g, carry):
                at = [q_ref[(o * steps + c) * chunk + g * 32 + j] for j in range(32)]
                got = [wide[pl.ds(q, parts, stride=8), :] for q in at]
                for j in range(32):
                    outs[pl.ds((g * 4 + j // 8) * 8 * parts + j % 8, parts, stride=8), :] = got[j]
                return carry

            lax.fori_loop(0, chunk // 32, rows, 0)

            @pl.when(c >= 2)
            def _():
                store(c - 2, slot).wait()

            def narrow(g, carry):
                for u in range(2):
                    base = (g * 4 + u * 2) * 8 * parts
                    v = [jnp.concatenate([outs[pl.ds(pl.multiple_of(base + (hh * parts + k) * 8, 8), 8), :] for hh in range(2)], axis=0) for k in range(parts)]
                    outbuf[slot, pl.ds(pl.multiple_of(g * 32 + u * 16, 16), 16), :] = jnp.concatenate(v, axis=1).astype(BF16)
                return carry

            lax.fori_loop(0, chunk // 32, narrow, 0)
            store(c, slot).start()
            return carry

        lax.fori_loop(0, steps, chunk_step, 0)
        for c in range(steps - 2, steps):
            store(c, c % 2).wait()

    for o, out in enumerate(results):
        fill(o, out)


def take_rows(tables, index, n_outs=1, chunk=512):
    rows_in = sum(t.shape[0] for t in tables)
    width = tables[0].shape[1]
    parts = width // 128
    rows_out = index.shape[0]
    q = (index // 8) * (8 * parts) + index % 8
    anyspec = pl.BlockSpec(memory_space=pl.ANY)
    return pl.pallas_call(
        functools.partial(take_body, len(tables), n_outs, rows_in, rows_out, chunk),
        grid_spec=pltpu.PrefetchScalarGridSpec(
            num_scalar_prefetch=1, grid=(1,), in_specs=[anyspec] * len(tables), out_specs=[anyspec] * n_outs,
            scratch_shapes=[pltpu.VMEM(((rows_in + 8) * parts, 128), F32), pltpu.VMEM((2, chunk, width), BF16),
                            pltpu.VMEM((chunk * parts, 128), F32), pltpu.VMEM((2, chunk, width), BF16),
                            pltpu.SemaphoreType.DMA((2,)), pltpu.SemaphoreType.DMA((2,))]),
        out_shape=[jax.ShapeDtypeStruct((rows_out // n_outs, width), BF16)] * n_outs,
        compiler_params=pltpu.CompilerParams(vmem_limit_bytes=VMEM_CAP),
        cost_estimate=pl.CostEstimate(flops=rows_out * 4096 * 8, bytes_accessed=2 * (rows_in + rows_out) * width, transcendentals=0),
        name="take_rows",
    )(q, *tables)


def join_body(*refs):
    pieces, outs, bufs, sems = refs[:8], refs[8:10], refs[10:12], refs[12:]
    mine = lax.axis_index("dp")
    copies = []
    for i, src in enumerate(pieces):
        kind, part, far = i // 4, (i // 2) % 2, i % 2
        owner = 1 - mine if far else mine
        rows, cols = src.shape
        dst = outs[0].at[owner, :, pl.ds(part * cols, cols)] if kind == 0 else outs[1].at[owner, pl.ds(part * rows, rows), :]
        buf = bufs[kind].at[i % 4]
        copies.append((pltpu.make_async_copy(src, buf, sems[0].at[i]), pltpu.make_async_copy(buf, dst, sems[1].at[i])))
    for c in copies:
        c[0].start()
    for c in copies:
        c[0].wait()
        c[1].start()
    for c in copies:
        c[1].wait()


def join_grads(near1, far1, near2, far2):
    width, part = near1[0].shape
    anyspec = pl.BlockSpec(memory_space=pl.ANY)
    pieces = [near1[0], far1[0], near1[1], far1[1], near2[0], far2[0], near2[1], far2[1]]
    return pl.pallas_call(
        join_body,
        in_specs=[anyspec] * 8,
        out_specs=[anyspec] * 2,
        out_shape=[jax.ShapeDtypeStruct((2, width, 2 * part), BF16), jax.ShapeDtypeStruct((2, 2 * part, width), BF16)],
        scratch_shapes=[pltpu.VMEM((4, width, part), BF16), pltpu.VMEM((4, part, width), BF16),
                        pltpu.SemaphoreType.DMA((8,)), pltpu.SemaphoreType.DMA((8,))],
        compiler_params=pltpu.CompilerParams(vmem_limit_bytes=40_000_000),
        cost_estimate=pl.CostEstimate(flops=10_000_000, bytes_accessed=16 * width * part * 2, transcendentals=0),
        name="join_grads",
    )(*pieces)


def exchange_body(ep_size, count, fchunk,
                  xo, dos, xs, ds, w1_hbm, w2_hbm, b1_ref, b2_ref, st_ref,
                  yb, dxb, dxl, g1a, g2a, g1b, g2b, p1a, p2a, gb1_ref, gb2_ref, st_out, dor, xr, dr, xf, df, yl, yol, dxol,
                  w1, w2, acc1, acc2, xv, dv, xt, dt, yacc, dxacc, ystage, dxstage, stage, slots,
                  st_send, st_recv, do_send, do_recv, x_send, x_recv, d_send, d_recv, xf_send, xf_recv, df_send, df_recv,
                  yo_send, yo_recv, dxo_send, dxo_recv, y_send, y_recv, g1_send, g1_recv, g2_send, g2_recv, w_sem, in_sem, out_sem, g_sem):
    width = w1.shape[0]
    hidden = w1.shape[1]
    mine, e = lax.axis_index("dp"), lax.axis_index("ep")
    me = mine * ep_size + e

    def anyone(k):
        p = lax.rem(me + k, count)
        return (p // ep_size, lax.rem(p, ep_size))

    def dest(k):
        return lax.rem(e + k, ep_size)

    def source(k):
        return lax.rem(e + ep_size - k, ep_size)

    def remote(src, dst, send, recv, dp, ep):
        return pltpu.make_async_remote_copy(src_ref=src, dst_ref=dst, send_sem=send, recv_sem=recv,
                                            device_id=(dp, ep), device_id_type=MESH_ID)

    def stat_copy(k):
        dp, ep = anyone(k)
        return remote(st_ref, slots.at[me], st_send.at[k], st_recv.at[k], dp, ep)

    def out_copy(src, dst, send, recv):
        return lambda k: remote(src.at[dest(k)], dst.at[e], send.at[k], recv.at[k], mine, dest(k))

    def back_copy(src, dst, base, send, recv):
        return lambda k: remote(src.at[source(k)], dst.at[base + e], send.at[k], recv.at[k], mine, source(k))

    do_copy = out_copy(dos, dor, do_send, do_recv)
    x_copy = out_copy(xs, xr, x_send, x_recv)
    d_copy = out_copy(ds, dr, d_send, d_recv)
    yo_copy = back_copy(yol, yb, 0, yo_send, yo_recv)
    dxo_copy = back_copy(dxol, dxb, 0, dxo_send, dxo_recv)
    y_copy = back_copy(yl, yb, ep_size, y_send, y_recv)

    def xf_copy(k):
        return remote(xo.at[source(k)], xf.at[source(k)], xf_send.at[k], xf_recv.at[k], 1 - mine, e)

    def df_copy(k):
        return remote(dor.at[source(k)], df.at[source(k)], df_send.at[k], df_recv.at[k], 1 - mine, e)

    def df_own():
        return remote(dos.at[e], df.at[e], df_send.at[0], df_recv.at[0], 1 - mine, e)

    def start_all(copies):
        for c in copies:
            c.start()

    def wait_all(copies):
        for c in copies:
            c.wait()

    def weights(which):
        return (pltpu.make_async_copy(w1_hbm.at[which], w1, w_sem.at[0]), pltpu.make_async_copy(w2_hbm.at[which], w2, w_sem.at[1]))

    def fetch(x_src, d_src, slot):
        return (pltpu.make_async_copy(x_src, xv.at[slot], in_sem.at[0, slot]),
                pltpu.make_async_copy(d_src, dv.at[slot], in_sem.at[1, slot]))

    def chunk(j, slot, which, want_rows, want_dw):
        cols = pl.ds(pl.multiple_of(j * fchunk, fchunk), fchunk)
        w1c = w1[:, cols]
        w2c = w2[cols, :]
        a = jnp.dot(xv[slot], w1c, preferred_element_type=F32) + b1_ref[which, :, cols].astype(F32)
        dh = lax.dot_general(dv[slot], w2c, (((1,), (1,)), ((), ())), preferred_element_type=F32)
        h, slope = gelu_and_slope(a)
        da = dh.astype(BF16).astype(F32) * slope
        h16 = h.astype(BF16)
        da16 = da.astype(BF16)
        if want_rows:
            yacc[...] += jnp.dot(h16, w2c, preferred_element_type=F32)
            dxacc[...] += lax.dot_general(da16, w1c, (((1,), (1,)), ((), ())), preferred_element_type=F32)
        if want_dw:
            gb1_ref[:, cols] += jnp.sum(da, axis=0, keepdims=True)
            acc1[:, cols] += jnp.dot(xt[...], da16, preferred_element_type=F32)
            acc2[:, cols] += jnp.dot(dt[...], h16, preferred_element_type=F32)

    def turn(slot):
        xt[...] = xv[slot].T
        dt[...] = dv[slot].T

    def add_bias_grad(slot):
        gb2_ref[...] += jnp.sum(dv[slot].astype(F32), axis=0, keepdims=True)

    def tile(slot, which, want_dw):
        if want_dw:
            turn(slot)
            add_bias_grad(slot)
        yacc[...] = jnp.broadcast_to(b2_ref[which].astype(F32), yacc.shape)
        dxacc[...] = jnp.zeros_like(dxacc)

        def step(j, carry):
            chunk(j, slot, which, True, want_dw)
            return carry

        lax.fori_loop(0, hidden // fchunk, step, 0)

    def put_rows(y_dst, dx_dst):
        return (pltpu.make_async_copy(ystage, y_dst, out_sem.at[0]), pltpu.make_async_copy(dxstage, dx_dst, out_sem.at[1]))

    start_all(weights(1 - mine))
    start_all(fetch(xo.at[e], dos.at[e], 0))
    barrier = pltpu.get_barrier_semaphore()
    for k in range(1, count):
        pl.semaphore_signal(barrier, inc=1, device_id=anyone(k), device_id_type=MESH_ID)
    pl.semaphore_wait(barrier, count - 1)
    for k in range(1, count):
        stat_copy(k).start()
    for k in range(1, ep_size):
        do_copy(k).start()
    df_own().start()
    for k in range(ep_size):
        xf_copy(k).start()
    for k in range(1, ep_size):
        x_copy(k).start()
        d_copy(k).start()
    slots[me] = st_ref[...]
    acc1[...] = jnp.zeros_like(acc1)
    acc2[...] = jnp.zeros_like(acc2)
    gb1_ref[...] = jnp.zeros_like(gb1_ref)
    gb2_ref[...] = jnp.zeros_like(gb2_ref)
    wait_all(weights(1 - mine))

    def other_step(k, carry):
        slot = lax.rem(k, 2)
        src = source(k)
        wait_all(fetch(xo.at[src], dos.at[src], slot))

        @pl.when(k < ep_size - 1)
        def _():
            do_copy(k + 1).wait_recv()
            df_copy(k + 1).start()
            start_all(fetch(xo.at[source(k + 1)], dor.at[source(k + 1)], lax.rem(k + 1, 2)))

        @pl.when(k >= 1)
        def _():
            wait_all(put_rows(yol.at[source(k - 1)], dxol.at[source(k - 1)]))

        @pl.when(k >= 2)
        def _():
            yo_copy(k - 1).start()
            dxo_copy(k - 1).start()

        tile(slot, 1 - mine, False)
        ystage[...] = yacc[...].astype(BF16)
        dxstage[...] = dxacc[...].astype(BF16)

        @pl.when(k == 0)
        def _():
            start_all(put_rows(yb.at[e], dxb.at[e]))

        @pl.when(k > 0)
        def _():
            start_all(put_rows(yol.at[src], dxol.at[src]))

        return carry

    last = ep_size - 1
    lax.fori_loop(0, ep_size, other_step, 0)
    start_all(weights(mine))
    start_all(fetch(xs.at[e], ds.at[e], 0))
    wait_all(put_rows(yol.at[source(last)], dxol.at[source(last)]))
    yo_copy(last).start()
    dxo_copy(last).start()
    wait_all(weights(mine))

    def near_step(k, carry):
        slot = lax.rem(k, 2)
        src = source(k)
        wait_all(fetch(xr.at[src], dr.at[src], slot))

        @pl.when(k < last)
        def _():
            x_copy(k + 1).wait_recv()
            d_copy(k + 1).wait_recv()
            start_all(fetch(xr.at[source(k + 1)], dr.at[source(k + 1)], lax.rem(k + 1, 2)))

        @pl.when(k >= 1)
        def _():
            wait_all(put_rows(yl.at[source(k - 1)], dxl.at[source(k - 1)]))

        @pl.when(k >= 2)
        def _():
            y_copy(k - 1).start()

        tile(slot, mine, True)
        ystage[...] = yacc[...].astype(BF16)
        dxstage[...] = dxacc[...].astype(BF16)

        @pl.when(k == 0)
        def _():
            start_all(put_rows(yb.at[ep_size + e], dxl.at[e]))

        @pl.when(k > 0)
        def _():
            start_all(put_rows(yl.at[src], dxl.at[src]))

        return carry

    lax.fori_loop(0, ep_size, near_step, 0)
    xf_copy(0).wait_recv()
    df_own().wait_recv()
    start_all(fetch(xf.at[e], df.at[e], 0))
    wait_all(put_rows(yl.at[source(last)], dxl.at[source(last)]))
    y_copy(last).start()

    chunks = hidden // fchunk
    early = chunks // 2
    half = early * fchunk

    def cols_of(j):
        return pl.ds(pl.multiple_of(j * fchunk, fchunk), fchunk)

    def grad_copies(j):
        return (remote(g1a.at[:, cols_of(j)], p1a.at[:, cols_of(j)], g1_send.at[j], g1_recv.at[j], 1 - mine, e),
                remote(g2a.at[cols_of(j), :], p2a.at[cols_of(j), :], g2_send.at[j], g2_recv.at[j], 1 - mine, e))

    def grad_out(j, late):
        if late:
            return (pltpu.make_async_copy(stage.at[0], g1b.at[:, cols_of(j - early)], g_sem.at[0]),
                    pltpu.make_async_copy(stage.at[1], g2b.at[cols_of(j - early), :], g_sem.at[1]))
        return (pltpu.make_async_copy(stage.at[0], g1a.at[:, cols_of(j)], g_sem.at[0]),
                pltpu.make_async_copy(stage.at[1], g2a.at[cols_of(j), :], g_sem.at[1]))

    def far_step(n, carry):
        j = n // ep_size
        k = lax.rem(n, ep_size)
        slot = lax.rem(n, 2)
        nxt = lax.rem(k + 1, ep_size)
        wait_all(fetch(xf.at[source(k)], df.at[source(k)], slot))

        @pl.when(n < last)
        def _():
            xf_copy(k + 1).wait_recv()
            df_copy(k + 1).wait_recv()

        @pl.when(n < chunks * ep_size - 1)
        def _():
            start_all(fetch(xf.at[source(nxt)], df.at[source(nxt)], lax.rem(n + 1, 2)))

        @pl.when((k == 1) & (j >= 1) & (j <= early))
        def _():
            wait_all(grad_out(j - 1, False))
            start_all(grad_copies(j - 1))

        @pl.when((k == 1) & (j > early))
        def _():
            wait_all(grad_out(j - 1, True))

        turn(slot)

        @pl.when(j == 0)
        def _():
            add_bias_grad(slot)

        chunk(j, slot, mine, False, True)

        @pl.when(k == last)
        def _():
            stage[0] = acc1[:, cols_of(j)].astype(BF16)
            stage[1] = acc2[:, cols_of(j)].T.astype(BF16)

        @pl.when((k == last) & (j < early))
        def _():
            start_all(grad_out(j, False))

        @pl.when((k == last) & (j >= early))
        def _():
            start_all(grad_out(j, True))

        return carry

    lax.fori_loop(0, chunks * ep_size, far_step, 0)
    wait_all(grad_out(chunks - 1, True))
    for j in range(early):
        wait_all(grad_copies(j))
    for k in range(1, count):
        stat_copy(k).wait()
    total = slots[0]
    for k in range(1, count):
        total = total + slots[k]
    st_out[...] = total
    df_own().wait_send()
    for k in range(ep_size):
        xf_copy(k).wait_send()
    for k in range(1, ep_size):
        df_copy(k).wait_send()
        do_copy(k).wait_send()
        x_copy(k).wait_send()
        d_copy(k).wait_send()
        yo_copy(k).wait()
        dxo_copy(k).wait()
        y_copy(k).wait()


def exchange_call(mesh, xo, dos, xs, ds, w1, b1, w2, b2, stats, fchunk=FCHUNK):
    ep_size = mesh.shape["ep"]
    count = mesh.shape["dp"] * ep_size
    tiles, r, width = xs.shape
    hidden = w1.shape[-1]
    anyspec = pl.BlockSpec(memory_space=pl.ANY)
    vm = pl.BlockSpec(memory_space=pltpu.VMEM)
    rows = jax.ShapeDtypeStruct(xs.shape, BF16)
    both = jax.ShapeDtypeStruct((2 * tiles, r, width), BF16)
    g1h = jax.ShapeDtypeStruct((width, hidden // 2), BF16)
    g2h = jax.ShapeDtypeStruct((hidden // 2, width), BF16)
    out_shape = [both, rows, rows, g1h, g2h, g1h, g2h, g1h, g2h,
                 jax.ShapeDtypeStruct((1, hidden), F32), jax.ShapeDtypeStruct((1, width), F32), jax.ShapeDtypeStruct(stats.shape, F32)] + [rows] * 8
    out_specs = [anyspec] * 9 + [vm] * 3 + [anyspec] * 8
    dma = pltpu.SemaphoreType.DMA
    scratch = [
        pltpu.VMEM((width, hidden), BF16), pltpu.VMEM((hidden, width), BF16),
        pltpu.VMEM((width, hidden), F32), pltpu.VMEM((width, hidden), F32),
        pltpu.VMEM((2, r, width), BF16), pltpu.VMEM((2, r, width), BF16),
        pltpu.VMEM((width, r), BF16), pltpu.VMEM((width, r), BF16),
        pltpu.VMEM((r, width), F32), pltpu.VMEM((r, width), F32),
        pltpu.VMEM((r, width), BF16), pltpu.VMEM((r, width), BF16),
        pltpu.VMEM((2, fchunk, width), BF16), pltpu.VMEM((count,) + stats.shape, F32),
        dma((count,)), dma((count,)),
    ] + [dma((ep_size,))] * 16 + [dma((hidden // fchunk,))] * 4 + [dma((2,)), dma((2, 2)), dma((2,)), dma((2,))]
    flops = 14 * 2 * tiles * r * width * hidden
    return pl.pallas_call(
        functools.partial(exchange_body, ep_size, count, fchunk),
        in_specs=[anyspec] * 6 + [vm] * 3,
        out_specs=out_specs,
        out_shape=out_shape,
        scratch_shapes=scratch,
        compiler_params=pltpu.CompilerParams(vmem_limit_bytes=VMEM_CAP, collective_id=1, has_side_effects=True),
        cost_estimate=pl.CostEstimate(flops=flops, bytes_accessed=12 * tiles * r * width * 2, transcendentals=3 * tiles * r * hidden),
        name="exchange",
    )(xo, dos, xs, ds, w1, w2, b1[:, None, :], b2[:, None, :], stats)[:12]


def router_forward(x_loc, modality, router, expert_ids):
    num_experts = router.shape[1]
    logits = jnp.dot(x_loc, router, precision=lax.Precision.HIGHEST, preferred_element_type=F32)
    log_probs = jax.nn.log_softmax(logits, axis=-1)
    router_probs = jnp.exp(log_probs)
    expert_onehot = (expert_ids[:, None] == jnp.arange(num_experts)[None, :]).astype(F32)
    gate_prob = jnp.sum(router_probs * expert_onehot, axis=-1)
    mod_mask = jnp.stack([modality == 0, modality == 1]).astype(F32)
    entropy = -jnp.sum(router_probs * log_probs, axis=-1)
    local_stats = jnp.concatenate([jnp.dot(mod_mask, router_probs), jnp.dot(mod_mask, entropy)[:, None], jnp.sum(mod_mask, axis=1, keepdims=True)], axis=1)
    return log_probs, router_probs, expert_onehot, gate_prob, mod_mask, local_stats


def aux_from_stats(stats, num_experts):
    mod_count = stats[:, num_experts + 1]
    mean_probs = stats[:, :num_experts] / mod_count[:, None]
    aux_loss = jnp.sum(stats[:, num_experts] / mod_count) + jnp.sum(mean_probs * jnp.log(mean_probs))
    return aux_loss, mean_probs, mod_count


def router_backward(x_loc, router, log_probs, router_probs, expert_onehot, mod_mask, mean_probs, mod_count, d_gate):
    inv_count = jnp.dot(1.0 / mod_count, mod_mask)
    global_part = jnp.einsum("mt,me->te", mod_mask, jnp.log(mean_probs) / mod_count[:, None])
    d_probs = expert_onehot * d_gate[:, None] + global_part - log_probs * inv_count[:, None]
    d_logits = router_probs * (d_probs - jnp.sum(d_probs * router_probs, axis=-1, keepdims=True))
    d_router_part = jnp.einsum("tw,te->we", x_loc, d_logits, precision=lax.Precision.HIGHEST, preferred_element_type=F32)
    dx_router = jnp.einsum("te,we->tw", d_logits, router, precision=lax.Precision.HIGHEST, preferred_element_type=F32)
    return d_router_part, dx_router.astype(BF16)


def solution(mesh):
    token_spec = P(ALL_AXES)
    expert_spec = P("ep")
    swap = [(i, 1 - i) for i in range(2)]

    def local_step(x_loc, modality, router, expert_ids, priority, w_in, b_in, w_out, b_out, dy_loc):
        num_tokens, width = x_loc.shape
        num_experts = router.shape[1]
        capacity = num_tokens // num_experts
        half = num_experts // 2
        mine = lax.axis_index("dp")
        order = jnp.argsort(expert_ids * num_tokens + priority)
        counts = jnp.sum((expert_ids[:, None] == jnp.arange(num_experts)[None, :]).astype(jnp.int32), axis=0)
        starts = jnp.cumsum(counts) - counts
        x_slots, d_slots = slot_tables(order, starts, counts, capacity)

        def to_owner(table, slots):
            rows = jnp.take(table, slots, axis=0, mode="clip").reshape(half, capacity, width)
            return lax.all_to_all(rows, "ep", 0, 0, tiled=True)

        def pick(table, slots):
            return [r.reshape(half, capacity, width) for r in take_rows([table], slots, n_outs=2)]

        def swap_rows(rows):
            return lax.all_to_all(rows, "ep", 0, 0, tiled=True)

        xo_rows, x_rows = pick(x_loc, x_slots)
        x_other = swap_rows(xo_rows)
        x_rt, _ = lax.optimization_barrier((x_loc, xo_rows))
        log_probs, router_probs, expert_onehot, gate_prob, mod_mask, local_stats = router_forward(x_rt, modality, router, expert_ids)
        dy_f32 = dy_loc.astype(F32)
        d_tok = (gate_prob[:, None] * dy_f32).astype(BF16)
        do_rows, d_rows = pick(d_tok, d_slots)
        stats_block = jnp.pad(local_stats, ((0, 6), (0, 128 - num_experts - 2)))
        y_back, dx_other, dx_mine, g_in0, g_out0, g_in1, g_out1, far_in0, far_out0, gb_in, gb_out, stats_sum = exchange_call(mesh, x_other, do_rows, x_rows, d_rows, w_in, b_in, w_out, b_out, stats_block)
        aux_loss, mean_probs, mod_count = aux_from_stats(stats_sum[:2, :num_experts + 2], num_experts)
        dx_back = [r.reshape(half * capacity, width) for r in (dx_other, swap_rows(dx_mine))]
        y_back = y_back.reshape(num_experts * capacity, width)
        g_bias = jnp.concatenate([gb_in, gb_out], axis=1).astype(BF16)
        far_out1 = lax.ppermute(g_out1, "dp", swap)
        far_in1 = lax.ppermute(g_in1, "dp", swap)
        far_bias = lax.ppermute(g_bias, "dp", swap)

        def both(near, far):
            first = mine == 0
            return jnp.stack([jnp.where(first, near, far), jnp.where(first, far, near)])

        rank = jnp.argsort(order)
        ids = jnp.arange(num_experts)
        position = rank - jnp.sum(jnp.where(expert_ids[:, None] == ids[None, :], starts[None, :], 0), axis=1)
        place = jnp.where(lax.rem(expert_ids, 2) == mine, half, 0) + expert_ids // 2
        token_slot = jnp.where(position < capacity, place * capacity + position, num_experts * capacity)

        y_tok = take_rows([y_back], token_slot)[0].astype(F32)
        out_tokens = (gate_prob[:, None] * y_tok).astype(BF16)
        d_gate = jnp.sum(dy_f32 * y_tok, axis=-1)
        d_router_part, dx_router = router_backward(x_loc, router, log_probs, router_probs, expert_onehot, mod_mask, mean_probs, mod_count, d_gate)
        dx_router = lax.optimization_barrier(dx_router)
        dx_tokens = take_rows(dx_back, token_slot)[0] + dx_router
        dx_tokens, d_router_part = lax.optimization_barrier((dx_tokens, d_router_part))
        d_router = device_sum(d_router_part.T.reshape(-1, 128), mesh, 2).reshape(num_experts, width).T
        d_router, far_in1, far_out1, far_bias = lax.optimization_barrier((d_router, far_in1, far_out1, far_bias))
        d_w_in, d_w_out = join_grads((g_in0, g_in1), (far_in0, far_in1), (g_out0, g_out1), (far_out0, far_out1))
        bias = both(g_bias[0], far_bias[0])
        hidden = w_in.shape[-1]
        return (out_tokens, aux_loss, dx_tokens, d_router, d_w_in, bias[:, :hidden], d_w_out, bias[:, hidden:])

    return jax.shard_map(
        local_step,
        mesh=mesh,
        in_specs=(token_spec, token_spec, P(), token_spec, token_spec, expert_spec, expert_spec, expert_spec, expert_spec, token_spec),
        out_specs=(token_spec, P(), token_spec, P(), expert_spec, expert_spec, expert_spec, expert_spec),
        check_vma=False,
    )
```

```python
import functools
import jax
import jax.numpy as jnp
from jax import lax
from jax.experimental import pallas as pl
from jax.experimental.pallas import tpu as pltpu
from jax.sharding import PartitionSpec as P


F32 = jnp.float32
BF16 = jnp.bfloat16
VMEM_CAP = 66_000_000
GELU_SCALE = 0.7978845608028654
GELU_CUBE = 0.044715
FCHUNK = 768


def gelu_and_slope(a):
    sq = a * a
    t = jnp.tanh(GELU_SCALE * (a + GELU_CUBE * (a * sq)))
    cdf = 0.5 * (1.0 + t)
    slope = cdf + (0.5 * a) * ((1.0 - t * t) * (GELU_SCALE * (1.0 + (3.0 * GELU_CUBE) * sq)))
    return a * cdf, slope


ALL_AXES = ("dp", "ep")
MESH_ID = pl.DeviceIdType.MESH


def slots_kernel(num_tokens, capacity, scal_ref, order_ref, xs_ref, ds_ref):
    mine = lax.axis_index("dp")
    experts = xs_ref.shape[0] * 128 // capacity
    rows = capacity // 128
    lane = lax.broadcasted_iota(jnp.int32, (rows, 128), 1)
    rank = lax.broadcasted_iota(jnp.int32, (rows, 128), 0) * 128 + lane
    for j in range(experts):
        owner = (1 - mine) if j < experts // 2 else mine
        e = 2 * (j % (experts // 2)) + owner
        start = scal_ref[e]
        count = scal_ref[experts + e]
        block = order_ref[pl.ds(start // 128, 8), :]
        off = lax.rem(start, 128)
        turned = pltpu.roll(block, lax.rem(128 - off, 128), 1)
        tok = jnp.where(lane < 128 - off, turned[:rows], turned[1:rows + 1])
        xs_ref[rows * j:rows * (j + 1), :] = jnp.where(rank < count, tok, 0)
        ds_ref[rows * j:rows * (j + 1), :] = jnp.where(rank < count, tok, num_tokens)


def slot_tables(order, starts, counts, capacity):
    num_tokens = order.shape[0]
    experts = starts.shape[0]
    padded = jnp.pad(order, (0, 1024)).reshape(-1, 128)
    shape = jax.ShapeDtypeStruct((experts * capacity // 128, 128), jnp.int32)
    xs, ds = pl.pallas_call(
        functools.partial(slots_kernel, num_tokens, capacity),
        in_specs=[pl.BlockSpec(memory_space=pltpu.SMEM), pl.BlockSpec(memory_space=pltpu.VMEM)],
        out_specs=[pl.BlockSpec(memory_space=pltpu.VMEM)] * 2,
        out_shape=[shape, shape],
        cost_estimate=pl.CostEstimate(flops=1_000_000, bytes_accessed=200_000, transcendentals=0),
        name="slots",
    )(jnp.concatenate([starts, counts]), padded)
    return xs.reshape(-1), ds.reshape(-1)


def sum_kernel(ep_size, count, x_ref, out_ref, slots, part, send_a, recv_a, send_b, recv_b):
    dp_me, ep_me = lax.axis_index("dp"), lax.axis_index("ep")
    me = dp_me * ep_size + ep_me

    def peer(k):
        return lax.rem(me + k, count)

    def to(src, dst, send, recv, p):
        return pltpu.make_async_remote_copy(src_ref=src, dst_ref=dst, send_sem=send, recv_sem=recv,
                                            device_id=(p // ep_size, lax.rem(p, ep_size)), device_id_type=MESH_ID)

    barrier = pltpu.get_barrier_semaphore()
    for k in range(1, count):
        p = peer(k)
        pl.semaphore_signal(barrier, inc=1, device_id=(p // ep_size, lax.rem(p, ep_size)), device_id_type=MESH_ID)
    pl.semaphore_wait(barrier, count - 1)
    scatter = [to(x_ref.at[peer(k)], slots.at[me], send_a.at[k], recv_a.at[k], peer(k)) for k in range(1, count)]
    for c in scatter:
        c.start()
    slots[me] = x_ref[me]
    for c in scatter:
        c.wait()
    total = slots[0]
    for k in range(1, count):
        total = total + slots[k]
    part[...] = total
    spread = [to(part, out_ref.at[me], send_b.at[k], recv_b.at[k], peer(k)) for k in range(1, count)]
    for c in spread:
        c.start()
    out_ref[me] = total
    for c in spread:
        c.wait()


def device_sum(x, mesh, collective_id):
    count = mesh.shape["dp"] * mesh.shape["ep"]
    dma = pltpu.SemaphoreType.DMA((count,))
    return pl.pallas_call(
        functools.partial(sum_kernel, mesh.shape["ep"], count),
        in_specs=[pl.BlockSpec(memory_space=pltpu.VMEM)],
        out_specs=pl.BlockSpec(memory_space=pltpu.VMEM),
        out_shape=jax.ShapeDtypeStruct(x.shape, F32),
        scratch_shapes=[pltpu.VMEM(x.shape, F32), pltpu.VMEM(x.shape[1:], F32), dma, dma, dma, dma],
        compiler_params=pltpu.CompilerParams(collective_id=collective_id, has_side_effects=True),
        cost_estimate=pl.CostEstimate(flops=10_000_000, bytes_accessed=1_000_000, transcendentals=0),
        name="device_sum",
    )(x)


def take_body(n_tables, n_outs, added, rows_in, rows_out, chunk, q_ref, *refs):
    tables, extra, results = refs[:n_tables], refs[n_tables:n_tables + added], refs[n_tables + added:n_tables + added + n_outs]
    wide, inbuf, outs, outbuf, in_sem, out_sem = refs[n_tables + added + n_outs:][:6]
    if added:
        addbuf, add_sem = refs[-2:]
    width = inbuf.shape[-1]
    parts = width // 128
    per_table = rows_in // chunk // n_tables

    def load(c):
        t, i = c // per_table, c % per_table
        return pltpu.make_async_copy(tables[t].at[pl.ds(i * chunk, chunk), :], inbuf.at[c % 2], in_sem.at[c % 2])

    load(0).start()
    for c in range(rows_in // chunk):
        if c + 1 < rows_in // chunk:
            load(c + 1).start()
        load(c).wait()

        def widen(g, carry, c=c):
            for u in range(4):
                v = inbuf[c % 2, pl.ds(pl.multiple_of(g * 64 + u * 16, 16), 16), :].astype(F32)
                base = (c * chunk // 8 + g * 8 + u * 2) * 8 * parts
                for hh in range(2):
                    for k in range(parts):
                        wide[pl.ds(pl.multiple_of(base + (hh * parts + k) * 8, 8), 8), :] = v[hh * 8:hh * 8 + 8, k * 128:(k + 1) * 128]
            return carry

        lax.fori_loop(0, chunk // 64, widen, 0)
    wide[rows_in * parts:, :] = jnp.zeros((8 * parts, 128), F32)

    steps = rows_out // chunk // n_outs

    def fill(o, out):
        def store(c, slot):
            return pltpu.make_async_copy(outbuf.at[slot], out.at[pl.ds(c * chunk, chunk), :], out_sem.at[slot])

        def addend(c, slot):
            return pltpu.make_async_copy(extra[0].at[pl.ds(c * chunk, chunk), :], addbuf.at[slot], add_sem.at[slot])

        if added:
            addend(0, 0).start()

        def chunk_step(c, carry):
            slot = lax.rem(c, 2)
            if added:
                @pl.when(c + 1 < steps)
                def _():
                    addend(c + 1, lax.rem(c + 1, 2)).start()

                addend(c, slot).wait()

            @pl.when(c >= 2)
            def _():
                store(c - 2, slot).wait()

            def rows(g):
                at = [q_ref[(o * steps + c) * chunk + g * 32 + j] for j in range(32)]
                got = [wide[pl.ds(q, parts, stride=8), :] for q in at]
                for j in range(32):
                    outs[pl.ds((g * 4 + j // 8) * 8 * parts + j % 8, parts, stride=8), :] = got[j]

            def narrow(g):
                for u in range(2):
                    base = (g * 4 + u * 2) * 8 * parts
                    v = [jnp.concatenate([outs[pl.ds(pl.multiple_of(base + (hh * parts + k) * 8, 8), 8), :] for hh in range(2)], axis=0) for k in range(parts)]
                    at = pl.ds(pl.multiple_of(g * 32 + u * 16, 16), 16)
                    row = jnp.concatenate(v, axis=1)
                    if added:
                        row = row + addbuf[slot, at, :].astype(F32)
                    outbuf[slot, at, :] = row.astype(BF16)

            def both_steps(g, carry):
                narrow(g - 1)
                rows(g)
                return carry

            rows(0)
            lax.fori_loop(1, chunk // 32, both_steps, 0)
            narrow(chunk // 32 - 1)
            store(c, slot).start()
            return carry

        lax.fori_loop(0, steps, chunk_step, 0)
        for c in range(steps - 2, steps):
            store(c, c % 2).wait()

    for o, out in enumerate(results):
        fill(o, out)


def take_rows(tables, index, n_outs=1, chunk=1024, addend=None):
    more = [] if addend is None else [addend]
    rows_in = sum(t.shape[0] for t in tables)
    width = tables[0].shape[1]
    parts = width // 128
    rows_out = index.shape[0]
    q = (index // 8) * (8 * parts) + index % 8
    anyspec = pl.BlockSpec(memory_space=pl.ANY)
    return pl.pallas_call(
        functools.partial(take_body, len(tables), n_outs, len(more), rows_in, rows_out, chunk),
        grid_spec=pltpu.PrefetchScalarGridSpec(
            num_scalar_prefetch=1, grid=(1,), in_specs=[anyspec] * (len(tables) + len(more)), out_specs=[anyspec] * n_outs,
            scratch_shapes=[pltpu.VMEM(((rows_in + 8) * parts, 128), F32), pltpu.VMEM((2, chunk, width), BF16),
                            pltpu.VMEM((chunk * parts, 128), F32), pltpu.VMEM((2, chunk, width), BF16),
                            pltpu.SemaphoreType.DMA((2,)), pltpu.SemaphoreType.DMA((2,))]
            + [pltpu.VMEM((2, chunk, width), BF16), pltpu.SemaphoreType.DMA((2,))] * len(more)),
        out_shape=[jax.ShapeDtypeStruct((rows_out // n_outs, width), BF16)] * n_outs,
        compiler_params=pltpu.CompilerParams(vmem_limit_bytes=VMEM_CAP),
        cost_estimate=pl.CostEstimate(flops=rows_out * 4096 * 8, bytes_accessed=2 * (rows_in + rows_out) * width, transcendentals=0),
        name="take_rows",
    )(q, *tables, *more)


def join_body(*refs):
    pieces, outs, bufs, sems = refs[:8], refs[8:10], refs[10:12], refs[12:]
    mine = lax.axis_index("dp")
    copies = []
    for i, src in enumerate(pieces):
        kind, part, far = i // 4, (i // 2) % 2, i % 2
        owner = 1 - mine if far else mine
        rows, cols = src.shape
        dst = outs[0].at[owner, :, pl.ds(part * cols, cols)] if kind == 0 else outs[1].at[owner, pl.ds(part * rows, rows), :]
        buf = bufs[kind].at[i % 4]
        copies.append((pltpu.make_async_copy(src, buf, sems[0].at[i]), pltpu.make_async_copy(buf, dst, sems[1].at[i])))
    for c in copies:
        c[0].start()
    for c in copies:
        c[0].wait()
        c[1].start()
    for c in copies:
        c[1].wait()


def join_grads(near1, far1, near2, far2):
    width, part = near1[0].shape
    anyspec = pl.BlockSpec(memory_space=pl.ANY)
    pieces = [near1[0], far1[0], near1[1], far1[1], near2[0], far2[0], near2[1], far2[1]]
    return pl.pallas_call(
        join_body,
        in_specs=[anyspec] * 8,
        out_specs=[anyspec] * 2,
        out_shape=[jax.ShapeDtypeStruct((2, width, 2 * part), BF16), jax.ShapeDtypeStruct((2, 2 * part, width), BF16)],
        scratch_shapes=[pltpu.VMEM((4, width, part), BF16), pltpu.VMEM((4, part, width), BF16),
                        pltpu.SemaphoreType.DMA((8,)), pltpu.SemaphoreType.DMA((8,))],
        compiler_params=pltpu.CompilerParams(vmem_limit_bytes=40_000_000),
        cost_estimate=pl.CostEstimate(flops=10_000_000, bytes_accessed=16 * width * part * 2, transcendentals=0),
        name="join_grads",
    )(*pieces)


def exchange_body(ep_size, count, fchunk,
                  xo, dos, xs, ds, w1_hbm, w2_hbm, b1_ref, b2_ref, st_ref,
                  yb, dxb, dxl, g1a, g2a, g1b, g2b, p1a, p2a, gb1_ref, gb2_ref, st_out, dor, xr, dr, xf, df, yl, yol, dxol,
                  w1, w2, acc1, acc2, xv, dv, xt, dt, yacc, dxacc, ystage, dxstage, stage, slots,
                  st_send, st_recv, do_send, do_recv, x_send, x_recv, d_send, d_recv, xf_send, xf_recv, df_send, df_recv,
                  yo_send, yo_recv, dxo_send, dxo_recv, y_send, y_recv, g1_send, g1_recv, g2_send, g2_recv, w_sem, in_sem, out_sem, g_sem):
    hidden = w1.shape[1]
    mine, e = lax.axis_index("dp"), lax.axis_index("ep")
    me = mine * ep_size + e

    def anyone(k):
        p = lax.rem(me + k, count)
        return (p // ep_size, lax.rem(p, ep_size))

    def dest(k):
        return lax.rem(e + k, ep_size)

    def source(k):
        return lax.rem(e + ep_size - k, ep_size)

    def remote(src, dst, send, recv, dp, ep):
        return pltpu.make_async_remote_copy(src_ref=src, dst_ref=dst, send_sem=send, recv_sem=recv,
                                            device_id=(dp, ep), device_id_type=MESH_ID)

    def stat_copy(k):
        dp, ep = anyone(k)
        return remote(st_ref, slots.at[me], st_send.at[k], st_recv.at[k], dp, ep)

    def out_copy(src, dst, send, recv):
        return lambda k: remote(src.at[dest(k)], dst.at[e], send.at[k], recv.at[k], mine, dest(k))

    def back_copy(src, dst, base, send, recv):
        return lambda k: remote(src.at[source(k)], dst.at[base + e], send.at[k], recv.at[k], mine, source(k))

    do_copy = out_copy(dos, dor, do_send, do_recv)
    x_copy = out_copy(xs, xr, x_send, x_recv)
    d_copy = out_copy(ds, dr, d_send, d_recv)
    yo_copy = back_copy(yol, yb, 0, yo_send, yo_recv)
    dxo_copy = back_copy(dxol, dxb, 0, dxo_send, dxo_recv)
    y_copy = back_copy(yl, yb, ep_size, y_send, y_recv)

    def xf_copy(k):
        return remote(xo.at[source(k)], xf.at[source(k)], xf_send.at[k], xf_recv.at[k], 1 - mine, e)

    def df_copy(k):
        return remote(dor.at[source(k)], df.at[source(k)], df_send.at[k], df_recv.at[k], 1 - mine, e)

    def df_own():
        return remote(dos.at[e], df.at[e], df_send.at[0], df_recv.at[0], 1 - mine, e)

    def start_all(copies):
        for c in copies:
            c.start()

    def wait_all(copies):
        for c in copies:
            c.wait()

    def weights(which):
        return (pltpu.make_async_copy(w1_hbm.at[which], w1, w_sem.at[0]), pltpu.make_async_copy(w2_hbm.at[which], w2, w_sem.at[1]))

    def fetch(x_src, d_src, slot):
        return (pltpu.make_async_copy(x_src, xv.at[slot], in_sem.at[0, slot]),
                pltpu.make_async_copy(d_src, dv.at[slot], in_sem.at[1, slot]))

    def chunk(j, slot, which, want_rows, want_dw):
        cols = pl.ds(pl.multiple_of(j * fchunk, fchunk), fchunk)
        w1c = w1[:, cols]
        w2c = w2[cols, :]
        a = jnp.dot(xv[slot], w1c, preferred_element_type=F32) + b1_ref[which, :, cols].astype(F32)
        dh = lax.dot_general(dv[slot], w2c, (((1,), (1,)), ((), ())), preferred_element_type=F32)
        h, slope = gelu_and_slope(a)
        da = dh.astype(BF16).astype(F32) * slope
        h16 = h.astype(BF16)
        da16 = da.astype(BF16)
        if want_rows:
            yacc[...] += jnp.dot(h16, w2c, preferred_element_type=F32)
            dxacc[...] += lax.dot_general(da16, w1c, (((1,), (1,)), ((), ())), preferred_element_type=F32)
        if want_dw:
            gb1_ref[:, cols] += jnp.sum(da, axis=0, keepdims=True)
            acc1[:, cols] += jnp.dot(xt[...], da16, preferred_element_type=F32)
            acc2[:, cols] += jnp.dot(dt[...], h16, preferred_element_type=F32)

    def turn(slot):
        xt[...] = xv[slot].T
        dt[...] = dv[slot].T

    def add_bias_grad(slot):
        gb2_ref[...] += jnp.sum(dv[slot].astype(F32), axis=0, keepdims=True)

    def tile(slot, which, want_dw):
        if want_dw:
            turn(slot)
            add_bias_grad(slot)
        yacc[...] = jnp.broadcast_to(b2_ref[which].astype(F32), yacc.shape)
        dxacc[...] = jnp.zeros_like(dxacc)

        def step(j, carry):
            chunk(j, slot, which, True, want_dw)
            return carry

        lax.fori_loop(0, hidden // fchunk, step, 0)

    def put_rows(y_dst, dx_dst):
        return (pltpu.make_async_copy(ystage, y_dst, out_sem.at[0]), pltpu.make_async_copy(dxstage, dx_dst, out_sem.at[1]))

    start_all(weights(1 - mine))
    start_all(fetch(xo.at[e], dos.at[e], 0))
    barrier = pltpu.get_barrier_semaphore()
    for k in range(1, count):
        pl.semaphore_signal(barrier, inc=1, device_id=anyone(k), device_id_type=MESH_ID)
    pl.semaphore_wait(barrier, count - 1)
    for k in range(1, count):
        stat_copy(k).start()
    for k in range(1, ep_size):
        do_copy(k).start()
    df_own().start()
    for k in range(ep_size):
        xf_copy(k).start()
    for k in range(1, ep_size):
        x_copy(k).start()
        d_copy(k).start()
    slots[me] = st_ref[...]
    acc1[...] = jnp.zeros_like(acc1)
    acc2[...] = jnp.zeros_like(acc2)
    gb1_ref[...] = jnp.zeros_like(gb1_ref)
    gb2_ref[...] = jnp.zeros_like(gb2_ref)
    wait_all(weights(1 - mine))

    def other_step(k, carry):
        slot = lax.rem(k, 2)
        src = source(k)
        wait_all(fetch(xo.at[src], dos.at[src], slot))

        @pl.when(k < ep_size - 1)
        def _():
            do_copy(k + 1).wait_recv()
            df_copy(k + 1).start()
            start_all(fetch(xo.at[source(k + 1)], dor.at[source(k + 1)], lax.rem(k + 1, 2)))

        @pl.when(k >= 1)
        def _():
            wait_all(put_rows(yol.at[source(k - 1)], dxol.at[source(k - 1)]))

        @pl.when(k >= 2)
        def _():
            yo_copy(k - 1).start()
            dxo_copy(k - 1).start()

        tile(slot, 1 - mine, False)
        ystage[...] = yacc[...].astype(BF16)
        dxstage[...] = dxacc[...].astype(BF16)

        @pl.when(k == 0)
        def _():
            start_all(put_rows(yb.at[e], dxb.at[e]))

        @pl.when(k > 0)
        def _():
            start_all(put_rows(yol.at[src], dxol.at[src]))

        return carry

    last = ep_size - 1
    lax.fori_loop(0, ep_size, other_step, 0)
    start_all(weights(mine))
    start_all(fetch(xs.at[e], ds.at[e], 0))
    wait_all(put_rows(yol.at[source(last)], dxol.at[source(last)]))
    yo_copy(last).start()
    dxo_copy(last).start()
    wait_all(weights(mine))

    def near_step(k, carry):
        slot = lax.rem(k, 2)
        src = source(k)
        wait_all(fetch(xr.at[src], dr.at[src], slot))

        @pl.when(k < last)
        def _():
            x_copy(k + 1).wait_recv()
            d_copy(k + 1).wait_recv()
            start_all(fetch(xr.at[source(k + 1)], dr.at[source(k + 1)], lax.rem(k + 1, 2)))

        @pl.when(k >= 1)
        def _():
            wait_all(put_rows(yl.at[source(k - 1)], dxl.at[source(k - 1)]))

        @pl.when(k >= 2)
        def _():
            y_copy(k - 1).start()

        tile(slot, mine, True)
        ystage[...] = yacc[...].astype(BF16)
        dxstage[...] = dxacc[...].astype(BF16)

        @pl.when(k == 0)
        def _():
            start_all(put_rows(yb.at[ep_size + e], dxl.at[e]))

        @pl.when(k > 0)
        def _():
            start_all(put_rows(yl.at[src], dxl.at[src]))

        return carry

    lax.fori_loop(0, ep_size, near_step, 0)
    xf_copy(0).wait_recv()
    df_own().wait_recv()
    start_all(fetch(xf.at[e], df.at[e], 0))
    wait_all(put_rows(yl.at[source(last)], dxl.at[source(last)]))
    y_copy(last).start()

    chunks = hidden // fchunk
    early = chunks // 2

    def cols_of(j):
        return pl.ds(pl.multiple_of(j * fchunk, fchunk), fchunk)

    def grad_copies(j):
        return (remote(g1a.at[:, cols_of(j)], p1a.at[:, cols_of(j)], g1_send.at[j], g1_recv.at[j], 1 - mine, e),
                remote(g2a.at[cols_of(j), :], p2a.at[cols_of(j), :], g2_send.at[j], g2_recv.at[j], 1 - mine, e))

    def grad_out(j, late):
        if late:
            return (pltpu.make_async_copy(stage.at[0], g1b.at[:, cols_of(j - early)], g_sem.at[0]),
                    pltpu.make_async_copy(stage.at[1], g2b.at[cols_of(j - early), :], g_sem.at[1]))
        return (pltpu.make_async_copy(stage.at[0], g1a.at[:, cols_of(j)], g_sem.at[0]),
                pltpu.make_async_copy(stage.at[1], g2a.at[cols_of(j), :], g_sem.at[1]))

    def far_step(n, carry):
        j = n // ep_size
        k = lax.rem(n, ep_size)
        slot = lax.rem(n, 2)
        nxt = lax.rem(k + 1, ep_size)
        wait_all(fetch(xf.at[source(k)], df.at[source(k)], slot))

        @pl.when(n < last)
        def _():
            xf_copy(k + 1).wait_recv()
            df_copy(k + 1).wait_recv()

        @pl.when(n < chunks * ep_size - 1)
        def _():
            start_all(fetch(xf.at[source(nxt)], df.at[source(nxt)], lax.rem(n + 1, 2)))

        @pl.when((k == 1) & (j >= 1) & (j <= early))
        def _():
            wait_all(grad_out(j - 1, False))
            start_all(grad_copies(j - 1))

        @pl.when((k == 1) & (j > early))
        def _():
            wait_all(grad_out(j - 1, True))

        turn(slot)

        @pl.when(j == 0)
        def _():
            add_bias_grad(slot)

        chunk(j, slot, mine, False, True)

        @pl.when(k == last)
        def _():
            stage[0] = acc1[:, cols_of(j)].astype(BF16)
            stage[1] = acc2[:, cols_of(j)].T.astype(BF16)

        @pl.when((k == last) & (j < early))
        def _():
            start_all(grad_out(j, False))

        @pl.when((k == last) & (j >= early))
        def _():
            start_all(grad_out(j, True))

        return carry

    lax.fori_loop(0, chunks * ep_size, far_step, 0)
    wait_all(grad_out(chunks - 1, True))
    for j in range(early):
        wait_all(grad_copies(j))
    for k in range(1, count):
        stat_copy(k).wait()
    total = slots[0]
    for k in range(1, count):
        total = total + slots[k]
    st_out[...] = total
    df_own().wait_send()
    for k in range(ep_size):
        xf_copy(k).wait_send()
    for k in range(1, ep_size):
        df_copy(k).wait_send()
        do_copy(k).wait_send()
        x_copy(k).wait_send()
        d_copy(k).wait_send()
        yo_copy(k).wait()
        dxo_copy(k).wait()
        y_copy(k).wait()


def exchange_call(mesh, xo, dos, xs, ds, w1, b1, w2, b2, stats, fchunk=FCHUNK):
    ep_size = mesh.shape["ep"]
    count = mesh.shape["dp"] * ep_size
    tiles, r, width = xs.shape
    hidden = w1.shape[-1]
    anyspec = pl.BlockSpec(memory_space=pl.ANY)
    vm = pl.BlockSpec(memory_space=pltpu.VMEM)
    rows = jax.ShapeDtypeStruct(xs.shape, BF16)
    both = jax.ShapeDtypeStruct((2 * tiles, r, width), BF16)
    g1h = jax.ShapeDtypeStruct((width, hidden // 2), BF16)
    g2h = jax.ShapeDtypeStruct((hidden // 2, width), BF16)
    out_shape = [both, rows, rows, g1h, g2h, g1h, g2h, g1h, g2h,
                 jax.ShapeDtypeStruct((1, hidden), F32), jax.ShapeDtypeStruct((1, width), F32), jax.ShapeDtypeStruct(stats.shape, F32)] + [rows] * 8
    out_specs = [anyspec] * 9 + [vm] * 3 + [anyspec] * 8
    dma = pltpu.SemaphoreType.DMA
    scratch = [
        pltpu.VMEM((width, hidden), BF16), pltpu.VMEM((hidden, width), BF16),
        pltpu.VMEM((width, hidden), F32), pltpu.VMEM((width, hidden), F32),
        pltpu.VMEM((2, r, width), BF16), pltpu.VMEM((2, r, width), BF16),
        pltpu.VMEM((width, r), BF16), pltpu.VMEM((width, r), BF16),
        pltpu.VMEM((r, width), F32), pltpu.VMEM((r, width), F32),
        pltpu.VMEM((r, width), BF16), pltpu.VMEM((r, width), BF16),
        pltpu.VMEM((2, fchunk, width), BF16), pltpu.VMEM((count,) + stats.shape, F32),
        dma((count,)), dma((count,)),
    ] + [dma((ep_size,))] * 16 + [dma((hidden // fchunk,))] * 4 + [dma((2,)), dma((2, 2)), dma((2,)), dma((2,))]
    flops = 14 * 2 * tiles * r * width * hidden
    return pl.pallas_call(
        functools.partial(exchange_body, ep_size, count, fchunk),
        in_specs=[anyspec] * 6 + [vm] * 3,
        out_specs=out_specs,
        out_shape=out_shape,
        scratch_shapes=scratch,
        compiler_params=pltpu.CompilerParams(vmem_limit_bytes=VMEM_CAP, collective_id=1, has_side_effects=True),
        cost_estimate=pl.CostEstimate(flops=flops, bytes_accessed=12 * tiles * r * width * 2, transcendentals=3 * tiles * r * hidden),
        name="exchange",
    )(xo, dos, xs, ds, w1, w2, b1[:, None, :], b2[:, None, :], stats)[:12]


def three_parts(v):
    high = lax.reduce_precision(v, 8, 7)
    rest = v - high
    mid = lax.reduce_precision(rest, 8, 7)
    return high.astype(BF16), mid.astype(BF16), (rest - mid).astype(BF16)


def router_forward(x_loc, modality, router, expert_ids):
    num_experts = router.shape[1]
    high, mid, low = three_parts(router)
    pieces = jnp.dot(x_loc, jnp.concatenate([high, mid, low], axis=1), preferred_element_type=F32)
    logits = (pieces[:, 2 * num_experts:] + pieces[:, num_experts:2 * num_experts]) + pieces[:, :num_experts]
    log_probs = jax.nn.log_softmax(logits, axis=-1)
    router_probs = jnp.exp(log_probs)
    expert_onehot = (expert_ids[:, None] == jnp.arange(num_experts)[None, :]).astype(F32)
    gate_prob = jnp.sum(router_probs * expert_onehot, axis=-1)
    mod_mask = jnp.stack([modality == 0, modality == 1]).astype(F32)
    entropy = -jnp.sum(router_probs * log_probs, axis=-1)
    local_stats = jnp.concatenate([jnp.dot(mod_mask, router_probs), jnp.dot(mod_mask, entropy)[:, None], jnp.sum(mod_mask, axis=1, keepdims=True)], axis=1)
    return log_probs, router_probs, expert_onehot, gate_prob, mod_mask, local_stats


def aux_from_stats(stats, num_experts):
    mod_count = stats[:, num_experts + 1]
    mean_probs = stats[:, :num_experts] / mod_count[:, None]
    aux_loss = jnp.sum(stats[:, num_experts] / mod_count) + jnp.sum(mean_probs * jnp.log(mean_probs))
    return aux_loss, mean_probs, mod_count


def router_backward(x_loc, router, log_probs, router_probs, expert_onehot, mod_mask, mean_probs, mod_count, d_gate):
    inv_count = jnp.dot(1.0 / mod_count, mod_mask)
    global_part = jnp.einsum("mt,me->te", mod_mask, jnp.log(mean_probs) / mod_count[:, None])
    d_probs = expert_onehot * d_gate[:, None] + global_part - log_probs * inv_count[:, None]
    d_logits = router_probs * (d_probs - jnp.sum(d_probs * router_probs, axis=-1, keepdims=True))
    num_experts = router.shape[1]
    d1, d2, d3 = three_parts(d_logits)
    r1, r2, r3 = three_parts(router)
    pieces = jnp.einsum("tw,te->we", x_loc, jnp.concatenate([d1, d2, d3], axis=1), preferred_element_type=F32)
    d_router_part = (pieces[:, 2 * num_experts:] + pieces[:, num_experts:2 * num_experts]) + pieces[:, :num_experts]
    d_wide = jnp.concatenate([d1, d1, d2, d2, d1, d3], axis=1)
    r_wide = jnp.concatenate([r1, r2, r1, r2, r3, r1], axis=1)
    dx_router = jnp.einsum("te,we->tw", d_wide, r_wide, preferred_element_type=F32)
    return d_router_part, dx_router.astype(BF16)


def solution(mesh):
    token_spec = P(ALL_AXES)
    expert_spec = P("ep")
    swap = [(i, 1 - i) for i in range(2)]

    def local_step(x_loc, modality, router, expert_ids, priority, w_in, b_in, w_out, b_out, dy_loc):
        num_tokens, width = x_loc.shape
        num_experts = router.shape[1]
        capacity = num_tokens // num_experts
        half = num_experts // 2
        mine = lax.axis_index("dp")
        order = jnp.argsort(expert_ids * num_tokens + priority)
        counts = jnp.sum((expert_ids[:, None] == jnp.arange(num_experts)[None, :]).astype(jnp.int32), axis=0)
        starts = jnp.cumsum(counts) - counts
        x_slots, d_slots = slot_tables(order, starts, counts, capacity)

        def pick(table, slots, n_outs):
            return [r.reshape(half, capacity, width) for r in take_rows([table], slots, n_outs=n_outs)]

        def swap_rows(rows):
            return lax.all_to_all(rows, "ep", 0, 0, tiled=True)

        first = half * capacity
        xo_rows = pick(x_loc, x_slots[:first], 1)[0]
        x_other = swap_rows(xo_rows)
        x_rt, _ = lax.optimization_barrier((x_loc, xo_rows))
        log_probs, router_probs, expert_onehot, gate_prob, mod_mask, local_stats = router_forward(x_rt, modality, router, expert_ids)
        dy_f32 = dy_loc.astype(F32)
        d_tok = (gate_prob[:, None] * dy_f32).astype(BF16)
        do_rows, d_rows = pick(d_tok, d_slots, 2)
        x_later, _ = lax.optimization_barrier((x_slots[first:], gate_prob))
        x_rows = pick(x_loc, x_later, 1)[0]
        stats_block = jnp.pad(local_stats, ((0, 6), (0, 128 - num_experts - 2)))
        rank = jnp.argsort(order)
        ids = jnp.arange(num_experts)
        position = rank - jnp.sum(jnp.where(expert_ids[:, None] == ids[None, :], starts[None, :], 0), axis=1)
        place = jnp.where(lax.rem(expert_ids, 2) == mine, half, 0) + expert_ids // 2
        token_slot = jnp.where(position < capacity, place * capacity + position, num_experts * capacity)
        stats_block, token_slot = lax.optimization_barrier((stats_block, token_slot))
        y_back, dx_other, dx_mine, g_in0, g_out0, g_in1, g_out1, far_in0, far_out0, gb_in, gb_out, stats_sum = exchange_call(mesh, x_other, do_rows, x_rows, d_rows, w_in, b_in, w_out, b_out, stats_block)
        aux_loss, mean_probs, mod_count = aux_from_stats(stats_sum[:2, :num_experts + 2], num_experts)
        dx_returned = swap_rows(dx_mine)
        dx_back = [r.reshape(half * capacity, width) for r in (dx_other, dx_returned)]
        y_back = y_back.reshape(num_experts * capacity, width)
        g_bias = jnp.concatenate([gb_in, gb_out], axis=1).astype(BF16)
        far_out1 = lax.ppermute(g_out1, "dp", swap)
        far_in1 = lax.ppermute(g_in1, "dp", swap)
        far_bias = lax.ppermute(g_bias, "dp", swap)

        def both(near, far):
            first = mine == 0
            return jnp.stack([jnp.where(first, near, far), jnp.where(first, far, near)])

        y_rows = take_rows([y_back], token_slot)[0]
        y_tok = y_rows.astype(F32)
        out_tokens = (gate_prob[:, None] * y_tok).astype(BF16)
        d_gate = jnp.sum(dy_f32 * y_tok, axis=-1)
        d_router_part, dx_router = router_backward(x_loc, router, log_probs, router_probs, expert_onehot, mod_mask, mean_probs, mod_count, d_gate)
        dx_tokens = take_rows(dx_back, token_slot, addend=dx_router)[0]
        dx_tokens, d_router_part = lax.optimization_barrier((dx_tokens, d_router_part))
        flat = d_router_part.T.reshape(-1, 128)
        blocks = jnp.pad(flat, ((0, mesh.size * 8 - flat.shape[0]), (0, 0))).reshape(mesh.size, 8, 128)
        d_router = device_sum(blocks, mesh, 2).reshape(-1, 128)[:flat.shape[0]].reshape(num_experts, width).T
        d_router, far_in1, far_out1, far_bias = lax.optimization_barrier((d_router, far_in1, far_out1, far_bias))
        d_w_in, d_w_out = join_grads((g_in0, g_in1), (far_in0, far_in1), (g_out0, g_out1), (far_out0, far_out1))
        bias = both(g_bias[0], far_bias[0])
        hidden = w_in.shape[-1]
        return (out_tokens, aux_loss, dx_tokens, d_router, d_w_in, bias[:, :hidden], d_w_out, bias[:, hidden:])

    return jax.shard_map(
        local_step,
        mesh=mesh,
        in_specs=(token_spec, token_spec, P(), token_spec, token_spec, expert_spec, expert_spec, expert_spec, expert_spec, token_spec),
        out_specs=(token_spec, P(), token_spec, P(), expert_spec, expert_spec, expert_spec, expert_spec),
        check_vma=False,
    )
```

```python
import functools
import jax
import jax.numpy as jnp
from jax import lax
from jax.experimental import pallas as pl
from jax.experimental.pallas import tpu as pltpu
from jax.sharding import PartitionSpec as P


F32 = jnp.float32
BF16 = jnp.bfloat16
VMEM_CAP = 66_000_000
GELU_SCALE = 0.7978845608028654
GELU_CUBE = 0.044715
FCHUNK = 768


def gelu_and_slope(a):
    sq = a * a
    t = jnp.tanh(GELU_SCALE * (a + GELU_CUBE * (a * sq)))
    cdf = 0.5 * (1.0 + t)
    slope = cdf + (0.5 * a) * ((1.0 - t * t) * (GELU_SCALE * (1.0 + (3.0 * GELU_CUBE) * sq)))
    return a * cdf, slope


ALL_AXES = ("dp", "ep")
MESH_ID = pl.DeviceIdType.MESH


def slots_kernel(num_tokens, capacity, scal_ref, order_ref, xs_ref, ds_ref):
    mine = lax.axis_index("dp")
    experts = xs_ref.shape[0] * 128 // capacity
    rows = capacity // 128
    lane = lax.broadcasted_iota(jnp.int32, (rows, 128), 1)
    rank = lax.broadcasted_iota(jnp.int32, (rows, 128), 0) * 128 + lane
    for j in range(experts):
        owner = (1 - mine) if j < experts // 2 else mine
        e = 2 * (j % (experts // 2)) + owner
        start = scal_ref[e]
        count = scal_ref[experts + e]
        block = order_ref[pl.ds(start // 128, 8), :]
        off = lax.rem(start, 128)
        turned = pltpu.roll(block, lax.rem(128 - off, 128), 1)
        tok = jnp.where(lane < 128 - off, turned[:rows], turned[1:rows + 1])
        xs_ref[rows * j:rows * (j + 1), :] = jnp.where(rank < count, tok, 0)
        ds_ref[rows * j:rows * (j + 1), :] = jnp.where(rank < count, tok, num_tokens)


def slot_tables(order, starts, counts, capacity):
    num_tokens = order.shape[0]
    experts = starts.shape[0]
    padded = jnp.pad(order, (0, 1024)).reshape(-1, 128)
    shape = jax.ShapeDtypeStruct((experts * capacity // 128, 128), jnp.int32)
    xs, ds = pl.pallas_call(
        functools.partial(slots_kernel, num_tokens, capacity),
        in_specs=[pl.BlockSpec(memory_space=pltpu.SMEM), pl.BlockSpec(memory_space=pltpu.VMEM)],
        out_specs=[pl.BlockSpec(memory_space=pltpu.VMEM)] * 2,
        out_shape=[shape, shape],
        cost_estimate=pl.CostEstimate(flops=1_000_000, bytes_accessed=200_000, transcendentals=0),
        name="slots",
    )(jnp.concatenate([starts, counts]), padded)
    return xs.reshape(-1), ds.reshape(-1)


def sum_kernel(ep_size, count, x_ref, out_ref, slots, part, send_a, recv_a, send_b, recv_b):
    dp_me, ep_me = lax.axis_index("dp"), lax.axis_index("ep")
    me = dp_me * ep_size + ep_me

    def peer(k):
        return lax.rem(me + k, count)

    def to(src, dst, send, recv, p):
        return pltpu.make_async_remote_copy(src_ref=src, dst_ref=dst, send_sem=send, recv_sem=recv,
                                            device_id=(p // ep_size, lax.rem(p, ep_size)), device_id_type=MESH_ID)

    barrier = pltpu.get_barrier_semaphore()
    for k in range(1, count):
        p = peer(k)
        pl.semaphore_signal(barrier, inc=1, device_id=(p // ep_size, lax.rem(p, ep_size)), device_id_type=MESH_ID)
    pl.semaphore_wait(barrier, count - 1)
    scatter = [to(x_ref.at[peer(k)], slots.at[me], send_a.at[k], recv_a.at[k], peer(k)) for k in range(1, count)]
    for c in scatter:
        c.start()
    slots[me] = x_ref[me]
    for c in scatter:
        c.wait()
    total = slots[0]
    for k in range(1, count):
        total = total + slots[k]
    part[...] = total
    spread = [to(part, out_ref.at[me], send_b.at[k], recv_b.at[k], peer(k)) for k in range(1, count)]
    for c in spread:
        c.start()
    out_ref[me] = total
    for c in spread:
        c.wait()


def device_sum(x, mesh, collective_id):
    count = mesh.shape["dp"] * mesh.shape["ep"]
    dma = pltpu.SemaphoreType.DMA((count,))
    return pl.pallas_call(
        functools.partial(sum_kernel, mesh.shape["ep"], count),
        in_specs=[pl.BlockSpec(memory_space=pltpu.VMEM)],
        out_specs=pl.BlockSpec(memory_space=pltpu.VMEM),
        out_shape=jax.ShapeDtypeStruct(x.shape, F32),
        scratch_shapes=[pltpu.VMEM(x.shape, F32), pltpu.VMEM(x.shape[1:], F32), dma, dma, dma, dma],
        compiler_params=pltpu.CompilerParams(collective_id=collective_id, has_side_effects=True),
        cost_estimate=pl.CostEstimate(flops=10_000_000, bytes_accessed=1_000_000, transcendentals=0),
        name="device_sum",
    )(x)


def take_body(n_tables, n_outs, added, rows_in, rows_out, chunk, q_ref, *refs):
    tables, extra, results = refs[:n_tables], refs[n_tables:n_tables + added], refs[n_tables + added:n_tables + added + n_outs]
    wide, inbuf, outs, outbuf, in_sem, out_sem = refs[n_tables + added + n_outs:][:6]
    if added:
        addbuf, add_sem = refs[-2:]
    width = inbuf.shape[-1]
    parts = width // 128
    per_table = rows_in // chunk // n_tables

    def load(c):
        t, i = c // per_table, c % per_table
        return pltpu.make_async_copy(tables[t].at[pl.ds(i * chunk, chunk), :], inbuf.at[c % 2], in_sem.at[c % 2])

    load(0).start()
    for c in range(rows_in // chunk):
        if c + 1 < rows_in // chunk:
            load(c + 1).start()
        load(c).wait()

        def widen(g, carry, c=c):
            for u in range(4):
                v = inbuf[c % 2, pl.ds(pl.multiple_of(g * 64 + u * 16, 16), 16), :].astype(F32)
                base = (c * chunk // 8 + g * 8 + u * 2) * 8 * parts
                for hh in range(2):
                    for k in range(parts):
                        wide[pl.ds(pl.multiple_of(base + (hh * parts + k) * 8, 8), 8), :] = v[hh * 8:hh * 8 + 8, k * 128:(k + 1) * 128]
            return carry

        lax.fori_loop(0, chunk // 64, widen, 0)
    wide[rows_in * parts:, :] = jnp.zeros((8 * parts, 128), F32)

    steps = rows_out // chunk // n_outs

    def fill(o, out):
        def store(c, slot):
            return pltpu.make_async_copy(outbuf.at[slot], out.at[pl.ds(c * chunk, chunk), :], out_sem.at[slot])

        def addend(c, slot):
            return pltpu.make_async_copy(extra[0].at[pl.ds(c * chunk, chunk), :], addbuf.at[slot], add_sem.at[slot])

        if added:
            addend(0, 0).start()

        def chunk_step(c, carry):
            slot = lax.rem(c, 2)
            if added:
                @pl.when(c + 1 < steps)
                def _():
                    addend(c + 1, lax.rem(c + 1, 2)).start()

                addend(c, slot).wait()

            @pl.when(c >= 2)
            def _():
                store(c - 2, slot).wait()

            def rows(g):
                at = [q_ref[(o * steps + c) * chunk + g * 32 + j] for j in range(32)]
                got = [wide[pl.ds(q, parts, stride=8), :] for q in at]
                for j in range(32):
                    outs[pl.ds((g * 4 + j // 8) * 8 * parts + j % 8, parts, stride=8), :] = got[j]

            def narrow(g):
                for u in range(2):
                    base = (g * 4 + u * 2) * 8 * parts
                    v = [jnp.concatenate([outs[pl.ds(pl.multiple_of(base + (hh * parts + k) * 8, 8), 8), :] for hh in range(2)], axis=0) for k in range(parts)]
                    at = pl.ds(pl.multiple_of(g * 32 + u * 16, 16), 16)
                    row = jnp.concatenate(v, axis=1)
                    if added:
                        row = row + addbuf[slot, at, :].astype(F32)
                    outbuf[slot, at, :] = row.astype(BF16)

            def both_steps(g, carry):
                narrow(g - 1)
                rows(g)
                return carry

            rows(0)
            lax.fori_loop(1, chunk // 32, both_steps, 0)
            narrow(chunk // 32 - 1)
            store(c, slot).start()
            return carry

        lax.fori_loop(0, steps, chunk_step, 0)
        for c in range(steps - 2, steps):
            store(c, c % 2).wait()

    for o, out in enumerate(results):
        fill(o, out)


def take_rows(tables, index, n_outs=1, chunk=1024, addend=None):
    more = [] if addend is None else [addend]
    rows_in = sum(t.shape[0] for t in tables)
    width = tables[0].shape[1]
    parts = width // 128
    rows_out = index.shape[0]
    q = (index // 8) * (8 * parts) + index % 8
    anyspec = pl.BlockSpec(memory_space=pl.ANY)
    return pl.pallas_call(
        functools.partial(take_body, len(tables), n_outs, len(more), rows_in, rows_out, chunk),
        grid_spec=pltpu.PrefetchScalarGridSpec(
            num_scalar_prefetch=1, grid=(1,), in_specs=[anyspec] * (len(tables) + len(more)), out_specs=[anyspec] * n_outs,
            scratch_shapes=[pltpu.VMEM(((rows_in + 8) * parts, 128), F32), pltpu.VMEM((2, chunk, width), BF16),
                            pltpu.VMEM((chunk * parts, 128), F32), pltpu.VMEM((2, chunk, width), BF16),
                            pltpu.SemaphoreType.DMA((2,)), pltpu.SemaphoreType.DMA((2,))]
            + [pltpu.VMEM((2, chunk, width), BF16), pltpu.SemaphoreType.DMA((2,))] * len(more)),
        out_shape=[jax.ShapeDtypeStruct((rows_out // n_outs, width), BF16)] * n_outs,
        compiler_params=pltpu.CompilerParams(vmem_limit_bytes=VMEM_CAP),
        cost_estimate=pl.CostEstimate(flops=rows_out * 4096 * 8, bytes_accessed=2 * (rows_in + rows_out) * width, transcendentals=0),
        name="take_rows",
    )(q, *tables, *more)


def join_body(places, count, *refs):
    pieces, outs, (bufs, sem_in, sem_out) = refs[:len(places)], refs[count:count + 2], refs[count + 2:]
    mine = lax.axis_index("dp")
    copies = []
    for i, (src, (kind, part, far)) in enumerate(zip(pieces, places)):
        owner = 1 - mine if far else mine
        rows, cols = src.shape
        dst = outs[0].at[owner, :, pl.ds(part * cols, cols)] if kind == 0 else outs[1].at[owner, pl.ds(part * rows, rows), :]
        buf = bufs.at[i, pl.ds(0, rows), pl.ds(0, cols)]
        copies.append((pltpu.make_async_copy(src, buf, sem_in.at[i]), pltpu.make_async_copy(buf, dst, sem_out.at[i])))
    for c in copies:
        c[0].start()
    for c in copies:
        c[0].wait()
        c[1].start()
    for c in copies:
        c[1].wait()


def join_grads(pieces, places, width, hidden, into=None):
    anyspec = pl.BlockSpec(memory_space=pl.ANY)
    held = [] if into is None else list(into)
    count = len(pieces) + len(held)
    part = hidden // 2
    side = max(width, part)
    return pl.pallas_call(
        functools.partial(join_body, places, count),
        in_specs=[anyspec] * count,
        out_specs=[anyspec] * 2,
        out_shape=[jax.ShapeDtypeStruct((2, width, hidden), BF16), jax.ShapeDtypeStruct((2, hidden, width), BF16)],
        input_output_aliases={len(pieces) + i: i for i in range(len(held))},
        scratch_shapes=[pltpu.VMEM((len(pieces), side, side), BF16),
                        pltpu.SemaphoreType.DMA((len(pieces),)), pltpu.SemaphoreType.DMA((len(pieces),))],
        compiler_params=pltpu.CompilerParams(vmem_limit_bytes=VMEM_CAP),
        cost_estimate=pl.CostEstimate(flops=10_000_000, bytes_accessed=4 * len(pieces) * width * part, transcendentals=0),
        name="join_grads",
    )(*pieces, *held)


def exchange_body(ep_size, count, fchunk,
                  xo, dos, xs, ds, w1_hbm, w2_hbm, b1_ref, b2_ref, st_ref,
                  yb, dxb, dxl, g1a, g2a, g1b, g2b, p1a, p2a, gb1_ref, gb2_ref, st_out, dor, xr, dr, xf, df, yl, yol, dxol,
                  w1, w2, acc1, acc2, xv, dv, xt, dt, yacc, dxacc, ystage, dxstage, stage, slots,
                  st_send, st_recv, do_send, do_recv, x_send, x_recv, d_send, d_recv, xf_send, xf_recv, df_send, df_recv,
                  yo_send, yo_recv, dxo_send, dxo_recv, y_send, y_recv, g1_send, g1_recv, g2_send, g2_recv, w_sem, in_sem, out_sem, g_sem):
    hidden = w1.shape[1]
    mine, e = lax.axis_index("dp"), lax.axis_index("ep")
    me = mine * ep_size + e

    def anyone(k):
        p = lax.rem(me + k, count)
        return (p // ep_size, lax.rem(p, ep_size))

    def dest(k):
        return lax.rem(e + k, ep_size)

    def source(k):
        return lax.rem(e + ep_size - k, ep_size)

    def remote(src, dst, send, recv, dp, ep):
        return pltpu.make_async_remote_copy(src_ref=src, dst_ref=dst, send_sem=send, recv_sem=recv,
                                            device_id=(dp, ep), device_id_type=MESH_ID)

    def stat_copy(k):
        dp, ep = anyone(k)
        return remote(st_ref, slots.at[me], st_send.at[k], st_recv.at[k], dp, ep)

    def out_copy(src, dst, send, recv):
        return lambda k: remote(src.at[dest(k)], dst.at[e], send.at[k], recv.at[k], mine, dest(k))

    def back_copy(src, dst, base, send, recv):
        return lambda k: remote(src.at[source(k)], dst.at[base + e], send.at[k], recv.at[k], mine, source(k))

    do_copy = out_copy(dos, dor, do_send, do_recv)
    x_copy = out_copy(xs, xr, x_send, x_recv)
    d_copy = out_copy(ds, dr, d_send, d_recv)
    yo_copy = back_copy(yol, yb, 0, yo_send, yo_recv)
    dxo_copy = back_copy(dxol, dxb, 0, dxo_send, dxo_recv)
    y_copy = back_copy(yl, yb, ep_size, y_send, y_recv)

    def xf_copy(k):
        return remote(xo.at[source(k)], xf.at[source(k)], xf_send.at[k], xf_recv.at[k], 1 - mine, e)

    def df_copy(k):
        return remote(dor.at[source(k)], df.at[source(k)], df_send.at[k], df_recv.at[k], 1 - mine, e)

    def df_own():
        return remote(dos.at[e], df.at[e], df_send.at[0], df_recv.at[0], 1 - mine, e)

    def start_all(copies):
        for c in copies:
            c.start()

    def wait_all(copies):
        for c in copies:
            c.wait()

    def weights(which):
        return (pltpu.make_async_copy(w1_hbm.at[which], w1, w_sem.at[0]), pltpu.make_async_copy(w2_hbm.at[which], w2, w_sem.at[1]))

    def fetch(x_src, d_src, slot):
        return (pltpu.make_async_copy(x_src, xv.at[slot], in_sem.at[0, slot]),
                pltpu.make_async_copy(d_src, dv.at[slot], in_sem.at[1, slot]))

    def chunk(j, slot, which, want_rows, want_dw):
        cols = pl.ds(pl.multiple_of(j * fchunk, fchunk), fchunk)
        w1c = w1[:, cols]
        w2c = w2[cols, :]
        a = jnp.dot(xv[slot], w1c, preferred_element_type=F32) + b1_ref[which, :, cols].astype(F32)
        dh = lax.dot_general(dv[slot], w2c, (((1,), (1,)), ((), ())), preferred_element_type=F32)
        h, slope = gelu_and_slope(a)
        da = dh.astype(BF16).astype(F32) * slope
        h16 = h.astype(BF16)
        da16 = da.astype(BF16)
        if want_rows:
            yacc[...] += jnp.dot(h16, w2c, preferred_element_type=F32)
            dxacc[...] += lax.dot_general(da16, w1c, (((1,), (1,)), ((), ())), preferred_element_type=F32)
        if want_dw:
            gb1_ref[:, cols] += jnp.sum(da, axis=0, keepdims=True)
            acc1[:, cols] += jnp.dot(xt[...], da16, preferred_element_type=F32)
            acc2[:, cols] += jnp.dot(dt[...], h16, preferred_element_type=F32)

    def turn(slot):
        xt[...] = xv[slot].T
        dt[...] = dv[slot].T

    def add_bias_grad(slot):
        gb2_ref[...] += jnp.sum(dv[slot].astype(F32), axis=0, keepdims=True)

    def tile(slot, which, want_dw):
        if want_dw:
            turn(slot)
            add_bias_grad(slot)
        yacc[...] = jnp.broadcast_to(b2_ref[which].astype(F32), yacc.shape)
        dxacc[...] = jnp.zeros_like(dxacc)

        def step(j, carry):
            chunk(j, slot, which, True, want_dw)
            return carry

        lax.fori_loop(0, hidden // fchunk, step, 0)

    def put_rows(y_dst, dx_dst):
        return (pltpu.make_async_copy(ystage, y_dst, out_sem.at[0]), pltpu.make_async_copy(dxstage, dx_dst, out_sem.at[1]))

    start_all(weights(1 - mine))
    start_all(fetch(xo.at[e], dos.at[e], 0))
    barrier = pltpu.get_barrier_semaphore()
    for k in range(1, count):
        pl.semaphore_signal(barrier, inc=1, device_id=anyone(k), device_id_type=MESH_ID)
    pl.semaphore_wait(barrier, count - 1)
    for k in range(1, count):
        stat_copy(k).start()
    for k in range(1, ep_size):
        do_copy(k).start()
    df_own().start()
    for k in range(ep_size):
        xf_copy(k).start()
    for k in range(1, ep_size):
        x_copy(k).start()
        d_copy(k).start()
    slots[me] = st_ref[...]
    acc1[...] = jnp.zeros_like(acc1)
    acc2[...] = jnp.zeros_like(acc2)
    gb1_ref[...] = jnp.zeros_like(gb1_ref)
    gb2_ref[...] = jnp.zeros_like(gb2_ref)
    wait_all(weights(1 - mine))

    def other_step(k, carry):
        slot = lax.rem(k, 2)
        src = source(k)
        wait_all(fetch(xo.at[src], dos.at[src], slot))

        @pl.when(k < ep_size - 1)
        def _():
            do_copy(k + 1).wait_recv()
            df_copy(k + 1).start()
            start_all(fetch(xo.at[source(k + 1)], dor.at[source(k + 1)], lax.rem(k + 1, 2)))

        @pl.when(k >= 1)
        def _():
            wait_all(put_rows(yol.at[source(k - 1)], dxol.at[source(k - 1)]))

        @pl.when(k >= 2)
        def _():
            yo_copy(k - 1).start()
            dxo_copy(k - 1).start()

        tile(slot, 1 - mine, False)
        ystage[...] = yacc[...].astype(BF16)
        dxstage[...] = dxacc[...].astype(BF16)

        @pl.when(k == 0)
        def _():
            start_all(put_rows(yb.at[e], dxb.at[e]))

        @pl.when(k > 0)
        def _():
            start_all(put_rows(yol.at[src], dxol.at[src]))

        return carry

    last = ep_size - 1
    lax.fori_loop(0, ep_size, other_step, 0)
    start_all(weights(mine))
    start_all(fetch(xs.at[e], ds.at[e], 0))
    wait_all(put_rows(yol.at[source(last)], dxol.at[source(last)]))
    yo_copy(last).start()
    dxo_copy(last).start()
    wait_all(weights(mine))

    def near_step(k, carry):
        slot = lax.rem(k, 2)
        src = source(k)
        wait_all(fetch(xr.at[src], dr.at[src], slot))

        @pl.when(k < last)
        def _():
            x_copy(k + 1).wait_recv()
            d_copy(k + 1).wait_recv()
            start_all(fetch(xr.at[source(k + 1)], dr.at[source(k + 1)], lax.rem(k + 1, 2)))

        @pl.when(k >= 1)
        def _():
            wait_all(put_rows(yl.at[source(k - 1)], dxl.at[source(k - 1)]))

        @pl.when(k >= 2)
        def _():
            y_copy(k - 1).start()

        tile(slot, mine, True)
        ystage[...] = yacc[...].astype(BF16)
        dxstage[...] = dxacc[...].astype(BF16)

        @pl.when(k == 0)
        def _():
            start_all(put_rows(yb.at[ep_size + e], dxl.at[e]))

        @pl.when(k > 0)
        def _():
            start_all(put_rows(yl.at[src], dxl.at[src]))

        return carry

    lax.fori_loop(0, ep_size, near_step, 0)
    xf_copy(0).wait_recv()
    df_own().wait_recv()
    start_all(fetch(xf.at[e], df.at[e], 0))
    wait_all(put_rows(yl.at[source(last)], dxl.at[source(last)]))
    y_copy(last).start()

    chunks = hidden // fchunk
    early = chunks // 2

    def cols_of(j):
        return pl.ds(pl.multiple_of(j * fchunk, fchunk), fchunk)

    def grad_copies(j):
        return (remote(g1a.at[:, cols_of(j)], p1a.at[:, cols_of(j)], g1_send.at[j], g1_recv.at[j], 1 - mine, e),
                remote(g2a.at[cols_of(j), :], p2a.at[cols_of(j), :], g2_send.at[j], g2_recv.at[j], 1 - mine, e))

    def grad_out(j, late):
        if late:
            return (pltpu.make_async_copy(stage.at[0], g1b.at[:, cols_of(j - early)], g_sem.at[0]),
                    pltpu.make_async_copy(stage.at[1], g2b.at[cols_of(j - early), :], g_sem.at[1]))
        return (pltpu.make_async_copy(stage.at[0], g1a.at[:, cols_of(j)], g_sem.at[0]),
                pltpu.make_async_copy(stage.at[1], g2a.at[cols_of(j), :], g_sem.at[1]))

    def far_step(n, carry):
        j = n // ep_size
        k = lax.rem(n, ep_size)
        slot = lax.rem(n, 2)
        nxt = lax.rem(k + 1, ep_size)
        wait_all(fetch(xf.at[source(k)], df.at[source(k)], slot))

        @pl.when(n < last)
        def _():
            xf_copy(k + 1).wait_recv()
            df_copy(k + 1).wait_recv()

        @pl.when(n < chunks * ep_size - 1)
        def _():
            start_all(fetch(xf.at[source(nxt)], df.at[source(nxt)], lax.rem(n + 1, 2)))

        @pl.when((k == 1) & (j >= 1) & (j <= early))
        def _():
            wait_all(grad_out(j - 1, False))
            start_all(grad_copies(j - 1))

        @pl.when((k == 1) & (j > early))
        def _():
            wait_all(grad_out(j - 1, True))

        turn(slot)

        @pl.when(j == 0)
        def _():
            add_bias_grad(slot)

        chunk(j, slot, mine, False, True)

        @pl.when(k == last)
        def _():
            stage[0] = acc1[:, cols_of(j)].astype(BF16)
            stage[1] = acc2[:, cols_of(j)].T.astype(BF16)

        @pl.when((k == last) & (j < early))
        def _():
            start_all(grad_out(j, False))

        @pl.when((k == last) & (j >= early))
        def _():
            start_all(grad_out(j, True))

        return carry

    lax.fori_loop(0, chunks * ep_size, far_step, 0)
    wait_all(grad_out(chunks - 1, True))
    for j in range(early):
        wait_all(grad_copies(j))
    for k in range(1, count):
        stat_copy(k).wait()
    total = slots[0]
    for k in range(1, count):
        total = total + slots[k]
    st_out[...] = total
    df_own().wait_send()
    for k in range(ep_size):
        xf_copy(k).wait_send()
    for k in range(1, ep_size):
        df_copy(k).wait_send()
        do_copy(k).wait_send()
        x_copy(k).wait_send()
        d_copy(k).wait_send()
        yo_copy(k).wait()
        dxo_copy(k).wait()
        y_copy(k).wait()


def exchange_call(mesh, xo, dos, xs, ds, w1, b1, w2, b2, stats, fchunk=FCHUNK):
    ep_size = mesh.shape["ep"]
    count = mesh.shape["dp"] * ep_size
    tiles, r, width = xs.shape
    hidden = w1.shape[-1]
    anyspec = pl.BlockSpec(memory_space=pl.ANY)
    vm = pl.BlockSpec(memory_space=pltpu.VMEM)
    rows = jax.ShapeDtypeStruct(xs.shape, BF16)
    both = jax.ShapeDtypeStruct((2 * tiles, r, width), BF16)
    g1h = jax.ShapeDtypeStruct((width, hidden // 2), BF16)
    g2h = jax.ShapeDtypeStruct((hidden // 2, width), BF16)
    out_shape = [both, rows, rows, g1h, g2h, g1h, g2h, g1h, g2h,
                 jax.ShapeDtypeStruct((1, hidden), F32), jax.ShapeDtypeStruct((1, width), F32), jax.ShapeDtypeStruct(stats.shape, F32)] + [rows] * 8
    out_specs = [anyspec] * 9 + [vm] * 3 + [anyspec] * 8
    dma = pltpu.SemaphoreType.DMA
    scratch = [
        pltpu.VMEM((width, hidden), BF16), pltpu.VMEM((hidden, width), BF16),
        pltpu.VMEM((width, hidden), F32), pltpu.VMEM((width, hidden), F32),
        pltpu.VMEM((2, r, width), BF16), pltpu.VMEM((2, r, width), BF16),
        pltpu.VMEM((width, r), BF16), pltpu.VMEM((width, r), BF16),
        pltpu.VMEM((r, width), F32), pltpu.VMEM((r, width), F32),
        pltpu.VMEM((r, width), BF16), pltpu.VMEM((r, width), BF16),
        pltpu.VMEM((2, fchunk, width), BF16), pltpu.VMEM((count,) + stats.shape, F32),
        dma((count,)), dma((count,)),
    ] + [dma((ep_size,))] * 16 + [dma((hidden // fchunk,))] * 4 + [dma((2,)), dma((2, 2)), dma((2,)), dma((2,))]
    flops = 14 * 2 * tiles * r * width * hidden
    return pl.pallas_call(
        functools.partial(exchange_body, ep_size, count, fchunk),
        in_specs=[anyspec] * 6 + [vm] * 3,
        out_specs=out_specs,
        out_shape=out_shape,
        scratch_shapes=scratch,
        compiler_params=pltpu.CompilerParams(vmem_limit_bytes=VMEM_CAP, collective_id=1, has_side_effects=True),
        cost_estimate=pl.CostEstimate(flops=flops, bytes_accessed=12 * tiles * r * width * 2, transcendentals=3 * tiles * r * hidden),
        name="exchange",
    )(xo, dos, xs, ds, w1, w2, b1[:, None, :], b2[:, None, :], stats)[:12]


def three_parts(v):
    high = lax.reduce_precision(v, 8, 7)
    rest = v - high
    mid = lax.reduce_precision(rest, 8, 7)
    return high.astype(BF16), mid.astype(BF16), (rest - mid).astype(BF16)


def router_forward(x_loc, modality, router, expert_ids):
    num_experts = router.shape[1]
    high, mid, low = three_parts(router)
    pieces = jnp.dot(x_loc, jnp.concatenate([high, mid, low], axis=1), preferred_element_type=F32)
    logits = (pieces[:, 2 * num_experts:] + pieces[:, num_experts:2 * num_experts]) + pieces[:, :num_experts]
    log_probs = jax.nn.log_softmax(logits, axis=-1)
    router_probs = jnp.exp(log_probs)
    expert_onehot = (expert_ids[:, None] == jnp.arange(num_experts)[None, :]).astype(F32)
    gate_prob = jnp.sum(router_probs * expert_onehot, axis=-1)
    mod_mask = jnp.stack([modality == 0, modality == 1]).astype(F32)
    entropy = -jnp.sum(router_probs * log_probs, axis=-1)
    local_stats = jnp.concatenate([jnp.dot(mod_mask, router_probs), jnp.dot(mod_mask, entropy)[:, None], jnp.sum(mod_mask, axis=1, keepdims=True)], axis=1)
    return log_probs, router_probs, expert_onehot, gate_prob, mod_mask, local_stats


def aux_from_stats(stats, num_experts):
    mod_count = stats[:, num_experts + 1]
    mean_probs = stats[:, :num_experts] / mod_count[:, None]
    aux_loss = jnp.sum(stats[:, num_experts] / mod_count) + jnp.sum(mean_probs * jnp.log(mean_probs))
    return aux_loss, mean_probs, mod_count


def router_backward(x_loc, router, log_probs, router_probs, expert_onehot, mod_mask, mean_probs, mod_count, d_gate):
    inv_count = jnp.dot(1.0 / mod_count, mod_mask)
    global_part = jnp.einsum("mt,me->te", mod_mask, jnp.log(mean_probs) / mod_count[:, None])
    d_probs = expert_onehot * d_gate[:, None] + global_part - log_probs * inv_count[:, None]
    d_logits = router_probs * (d_probs - jnp.sum(d_probs * router_probs, axis=-1, keepdims=True))
    num_experts = router.shape[1]
    d1, d2, d3 = three_parts(d_logits)
    r1, r2, r3 = three_parts(router)
    pieces = jnp.einsum("tw,te->we", x_loc, jnp.concatenate([d1, d2, d3], axis=1), preferred_element_type=F32)
    d_router_part = (pieces[:, 2 * num_experts:] + pieces[:, num_experts:2 * num_experts]) + pieces[:, :num_experts]
    d_wide = jnp.concatenate([d1, d1, d2, d2, d1, d3], axis=1)
    r_wide = jnp.concatenate([r1, r2, r1, r2, r3, r1], axis=1)
    dx_router = jnp.einsum("te,we->tw", d_wide, r_wide, preferred_element_type=F32)
    return d_router_part, dx_router.astype(BF16)


def solution(mesh):
    token_spec = P(ALL_AXES)
    expert_spec = P("ep")
    swap = [(i, 1 - i) for i in range(2)]

    def local_step(x_loc, modality, router, expert_ids, priority, w_in, b_in, w_out, b_out, dy_loc):
        num_tokens, width = x_loc.shape
        num_experts = router.shape[1]
        capacity = num_tokens // num_experts
        half = num_experts // 2
        mine = lax.axis_index("dp")
        order = jnp.argsort(expert_ids * num_tokens + priority)
        counts = jnp.sum((expert_ids[:, None] == jnp.arange(num_experts)[None, :]).astype(jnp.int32), axis=0)
        starts = jnp.cumsum(counts) - counts
        x_slots, d_slots = slot_tables(order, starts, counts, capacity)

        def pick(table, slots, n_outs):
            return [r.reshape(half, capacity, width) for r in take_rows([table], slots, n_outs=n_outs)]

        def swap_rows(rows):
            return lax.all_to_all(rows, "ep", 0, 0, tiled=True)

        first = half * capacity
        xo_rows = pick(x_loc, x_slots[:first], 1)[0]
        x_other = swap_rows(xo_rows)
        x_rt, _ = lax.optimization_barrier((x_loc, xo_rows))
        log_probs, router_probs, expert_onehot, gate_prob, mod_mask, local_stats = router_forward(x_rt, modality, router, expert_ids)
        dy_f32 = dy_loc.astype(F32)
        d_tok = (gate_prob[:, None] * dy_f32).astype(BF16)
        do_rows, d_rows = pick(d_tok, d_slots, 2)
        x_later, _ = lax.optimization_barrier((x_slots[first:], gate_prob))
        x_rows = pick(x_loc, x_later, 1)[0]
        stats_block = jnp.pad(local_stats, ((0, 6), (0, 128 - num_experts - 2)))
        rank = jnp.argsort(order)
        ids = jnp.arange(num_experts)
        position = rank - jnp.sum(jnp.where(expert_ids[:, None] == ids[None, :], starts[None, :], 0), axis=1)
        place = jnp.where(lax.rem(expert_ids, 2) == mine, half, 0) + expert_ids // 2
        token_slot = jnp.where(position < capacity, place * capacity + position, num_experts * capacity)
        stats_block, token_slot = lax.optimization_barrier((stats_block, token_slot))
        y_back, dx_other, dx_mine, g_in0, g_out0, g_in1, g_out1, far_in0, far_out0, gb_in, gb_out, stats_sum = exchange_call(mesh, x_other, do_rows, x_rows, d_rows, w_in, b_in, w_out, b_out, stats_block)
        aux_loss, mean_probs, mod_count = aux_from_stats(stats_sum[:2, :num_experts + 2], num_experts)
        dx_returned = swap_rows(dx_mine)
        dx_back = [r.reshape(half * capacity, width) for r in (dx_other, dx_returned)]
        y_back = y_back.reshape(num_experts * capacity, width)
        g_bias = jnp.concatenate([gb_in, gb_out], axis=1).astype(BF16)
        far_out1 = lax.ppermute(g_out1, "dp", swap)
        far_in1 = lax.ppermute(g_in1, "dp", swap)
        far_bias = lax.ppermute(g_bias, "dp", swap)

        def both(near, far):
            first = mine == 0
            return jnp.stack([jnp.where(first, near, far), jnp.where(first, far, near)])

        y_rows = take_rows([y_back], token_slot)[0]
        y_tok = y_rows.astype(F32)
        joined = join_grads([g_in0, far_in0, g_in1, g_out0, far_out0, g_out1],
                            ((0, 0, False), (0, 0, True), (0, 1, False), (1, 0, False), (1, 0, True), (1, 1, False)), width, w_in.shape[-1])
        out_tokens = (gate_prob[:, None] * y_tok).astype(BF16)
        d_gate = jnp.sum(dy_f32 * y_tok, axis=-1)
        d_router_part, dx_router = router_backward(x_loc, router, log_probs, router_probs, expert_onehot, mod_mask, mean_probs, mod_count, d_gate)
        dx_tokens = take_rows(dx_back, token_slot, addend=dx_router)[0]
        dx_tokens, d_router_part = lax.optimization_barrier((dx_tokens, d_router_part))
        flat = d_router_part.T.reshape(-1, 128)
        blocks = jnp.pad(flat, ((0, mesh.size * 8 - flat.shape[0]), (0, 0))).reshape(mesh.size, 8, 128)
        d_router = device_sum(blocks, mesh, 2).reshape(-1, 128)[:flat.shape[0]].reshape(num_experts, width).T
        d_router, far_in1, far_out1, far_bias = lax.optimization_barrier((d_router, far_in1, far_out1, far_bias))
        hidden = w_in.shape[-1]
        d_w_in, d_w_out = join_grads([far_in1, far_out1], ((0, 1, True), (1, 1, True)), width, hidden, into=joined)
        bias = both(g_bias[0], far_bias[0])
        hidden = w_in.shape[-1]
        return (out_tokens, aux_loss, dx_tokens, d_router, d_w_in, bias[:, :hidden], d_w_out, bias[:, hidden:])

    return jax.shard_map(
        local_step,
        mesh=mesh,
        in_specs=(token_spec, token_spec, P(), token_spec, token_spec, expert_spec, expert_spec, expert_spec, expert_spec, token_spec),
        out_specs=(token_spec, P(), token_spec, P(), expert_spec, expert_spec, expert_spec, expert_spec),
        check_vma=False,
    )
```
